32 devices in a mesh: dp: 2 (over x), expert: 16 (over z, y, core).
Axes of the slice: x: 2, y: 2, z: 4, core: 2. Of those that a mesh axis runs over, the one named last changes fastest.
Arguments:
- tokens: bfloat16 [4096, 2048], P(('dp', 'expert')), may hold values from -6 to 6
- grad_out: bfloat16 [4096, 2048], P(('dp', 'expert')), may hold values from -0.125 to 0.125
- router_weight: bfloat16 [2048, 16], replicated, may hold values from -0.125 to 0.125
- expert_index: int32 [4096, 8], P(('dp', 'expert')), may hold values from 0 to 15, all different within a row; in each aligned block of 128 rows (0 to 127, 128 to 255, ...) at most 96 rows name the same one
- w_gate: bfloat16 [16, 2048, 768], P('expert'), may hold values from -0.125 to 0.125
- w_up: bfloat16 [16, 2048, 768], P('expert'), may hold values from -0.125 to 0.125
- w_down: bfloat16 [16, 768, 2048], P('expert'), may hold values from -0.21875 to 0.21875
Outputs:
- gate_grad: float32 [4096, 8], P(('dp', 'expert'))
- router_grad: float32 [2048, 16], P('expert')
The draws below stay inside these ranges and needn't reach their ends.
Inputs may be any that keep to these rules, and one draw needn't show every extreme that they name: `expert_index`: each row names 8 different experts. In each aligned block of 128 rows (the rows of one device) no expert is named by more than 96 rows, a bound that some blocks reach.
All inputs are finite; a program needn't handle non-finite values.
Results may differ from the reference program's by a relative error of at most 0.009.
Values may be sent and summed in bfloat16 or wider, within the bound.
A program may use at most 128 MiB of HBM per device.

```python
import math
import jax
import jax.numpy as jnp
import numpy as np
from jax import lax

D = 2048
FF = 768
TOP = 8
TOK_DEV = 128
EXPERTS = 16
CAP = 96
TOKENS = 4096


def spiked(array, stream_key, source, target, shards_of, factor):
    def block_of(position):
        return (jnp.arange(array.shape[position]) // (array.shape[position] // shards_of)).reshape((-1,) + (1,) * (array.ndim - 1 - position))

    one_side = jax.random.permutation(stream_key, shards_of)[block_of(target)]
    second = (block_of(target) + shards_of // 2) % shards_of
    return jnp.where((block_of(source) == one_side) | (block_of(source) == second), factor * array, array)


def steps_of(stream_key, dims, shards, least, high):
    loudness = 1.0
    for dim, parts in shards:
        heights = jax.random.uniform(jax.random.fold_in(jax.random.fold_in(stream_key, 6), dim), (parts,), jnp.float32, least / len(shards), high / len(shards))
        loudness = loudness * jnp.repeat(jnp.exp(heights), dims[dim] // parts).reshape((-1,) + (1,) * (len(dims) - 1 - dim))
    return loudness


def deal_out(rng, own, number, rows, count, top, most, slope):
    ranking = jax.random.permutation(rng, count)
    heavy_load, common = portions_of(count, rows * top, most, slope, True), portions_of(count, rows * top, most, slope, False)
    places = jnp.arange(count)

    def named(sizes, rotation):
        used = int((sizes > 0).sum())
        fixed = max(1, used // 4)
        shifted = fixed + (places - fixed + rotation * (used - fixed)) % max(1, count - fixed)
        return jnp.zeros((count,), jnp.int32).at[ranking[jnp.where(places < fixed, places, shifted)]].set(jnp.asarray(sizes, jnp.int32))

    sizes = jnp.where(number % 4 == 0, named(heavy_load, number // 4), named(common, number - number // 4 - 1))
    mixed = jax.random.permutation(jax.random.fold_in(own, 3), count)
    donor, taker = mixed[0:count // 2 * 2:2], mixed[1:count // 2 * 2:2]
    margin = jnp.minimum(sizes[donor] - 1, most - sizes[taker]) // 2
    margin = jnp.where((donor == ranking[0]) | (taker == ranking[0]) | (sizes[taker] == 0), 0, jnp.maximum(margin, 0))
    shifted = jax.random.randint(jax.random.fold_in(own, 4), (count // 2,), 0, 1 << 20) % (margin + 1)
    sizes = sizes.at[donor].add(-shifted).at[taker].add(shifted)
    items = jnp.searchsorted(jnp.cumsum(sizes), jnp.arange(rows * top), side="right").astype(jnp.int32)
    listing = items.reshape(top, rows).T
    listing = listing[jax.random.permutation(jax.random.fold_in(own, 1), rows)]
    rotation = jax.random.randint(jax.random.fold_in(own, 2), (rows, 1), 0, top)
    return jnp.take_along_axis(listing, (jnp.arange(top)[None, :] + rotation) % top, axis=1)


def portions_of(number_of, total, bound, slope, full):
    weights = [(1 << 20) // math.isqrt(standing ** slope) + 1 for standing in range(1, number_of + 1)]
    largest = bound if full else min(bound, max(-(-total // number_of), total * weights[0] // sum(weights)))
    least = 1 if total - largest >= number_of - 1 else 0
    counts, rest = [largest] + [least] * (number_of - 1), total - largest - least * (number_of - 1)
    while rest > 0:
        movable = [i for i in range(1, number_of) if counts[i] < largest] or [i for i in range(1, number_of) if counts[i] < bound]
        whole, remaining = sum([weights[i] for i in movable]), rest
        for i in movable:
            extra = min(bound - counts[i], max(1, remaining * weights[i] // whole), rest)
            counts[i] = counts[i] + extra
            rest = rest - extra
    return np.array(counts)


def bell_draw(stream_key, dims, width, most, pieces=(), held_as=jnp.bfloat16):
    gain = steps_of(stream_key, dims, pieces, -0.22, 0.18) if pieces else 1.0
    result = jax.random.normal(stream_key, dims, jnp.float32) * width * gain
    return jnp.minimum(jnp.maximum(result, -most), most).astype(held_as)


def gaussian_with(key, extent, spread, bound, shards, heavy, held_as=jnp.bfloat16):
    values = spread * jax.random.normal(key, extent, jnp.float32)
    if shards:
        values = values * steps_of(key, extent, shards, -0.22, 0.18)
    return jnp.clip(spiked(values, jax.random.fold_in(key, 3), *heavy), -bound, bound).astype(held_as)


def setup_inputs(seed: int = 0) -> dict:
    keys = jax.random.split(jax.random.key(seed), 8)
    tokens = gaussian_with(keys[0], (TOKENS, D), 1.0, 6.0, ((0, 32),), (0, 1, 32, 2.75))
    grad_out = bell_draw(keys[1], (TOKENS, D), D ** -0.5, 0.125, ((0, 32),))
    router_weight = bell_draw(keys[2], (D, EXPERTS), D ** -0.5, 0.125)
    expert_index_keys = jax.random.split(jax.random.fold_in(keys[3], 1), TOKENS // TOK_DEV)
    expert_index_turns = jax.random.permutation(jax.random.fold_in(keys[3], 3), TOKENS // TOK_DEV)
    expert_index = jax.vmap(lambda own, number: deal_out(jax.random.fold_in(keys[3], 2), own, number, TOK_DEV, EXPERTS, TOP, CAP, 2))(expert_index_keys, expert_index_turns).reshape((TOKENS, TOP))
    w_gate = bell_draw(keys[4], (EXPERTS, D, FF), D ** -0.5, 0.125, ((0, 16),))
    w_up = bell_draw(keys[5], (EXPERTS, D, FF), D ** -0.5, 0.125, ((0, 16),))
    w_down = bell_draw(keys[6], (EXPERTS, FF, D), FF ** -0.5, 0.21875, ((0, 16),))
    return dict(tokens=tokens, grad_out=grad_out, router_weight=router_weight, expert_index=expert_index, w_gate=w_gate, w_up=w_up, w_down=w_down)


def slot_table(expert_index):
    blocks = expert_index.reshape(-1, TOK_DEV, TOP)
    labels = jnp.arange(EXPERTS, dtype=jnp.int32)
    hits = (blocks[..., None] == labels).astype(jnp.int32)
    per_token = jnp.sum(hits, axis=2)
    before = jnp.cumsum(per_token, axis=1) - per_token
    slot = jnp.sum(hits * before[:, :, None, :], axis=3)
    return slot.reshape(-1, TOP).astype(jnp.int32)


def reference(tokens, grad_out, router_weight, expert_index, w_gate, w_up, w_down):
    slot = slot_table(expert_index)
    blocks = TOKENS // TOK_DEV
    token_ids = jnp.broadcast_to(jnp.arange(TOKENS, dtype=jnp.int32)[:, None], (TOKENS, TOP))
    source = (token_ids // TOK_DEV).astype(jnp.int32)
    column = (source * CAP + slot).astype(jnp.int32)
    table = jnp.zeros((EXPERTS, blocks * CAP), jnp.int32).at[expert_index, column].set(token_ids)

    def one_expert(which):
        picked = table[which]
        rows = tokens[picked]
        gate_in = jnp.dot(rows, w_gate[which], preferred_element_type=jnp.float32)
        up_in = jnp.dot(rows, w_up[which], preferred_element_type=jnp.float32)
        hidden = (jax.nn.silu(gate_in) * up_in).astype(jnp.bfloat16)
        expert_out = jnp.dot(hidden, w_down[which], preferred_element_type=jnp.float32).astype(jnp.bfloat16)
        return jnp.sum(expert_out.astype(jnp.float32) * grad_out[picked].astype(jnp.float32), axis=1)

    dots = lax.map(one_expert, jnp.arange(EXPERTS, dtype=jnp.int32))
    gate_grad = dots[expert_index, column]

    logits = jnp.dot(tokens, router_weight, preferred_element_type=jnp.float32)
    chosen = jnp.take_along_axis(logits, expert_index, axis=1)
    weights = jnp.exp(chosen)
    gates = weights / jnp.sum(weights, axis=1, keepdims=True)
    mean_term = jnp.sum(gates * gate_grad, axis=1, keepdims=True)
    logit_grad = gates * (gate_grad - mean_term)
    labels = jnp.arange(EXPERTS, dtype=jnp.int32)
    hits = (expert_index[:, :, None] == labels).astype(jnp.float32)
    dense = jnp.sum(logit_grad[:, :, None] * hits, axis=1)
    router_grad = jnp.dot(tokens.astype(jnp.float32).T, dense, precision=lax.Precision.HIGHEST)
    return gate_grad, router_grad
```

```python
import functools

import jax
import jax.numpy as jnp
from jax import lax
from jax.experimental import pallas as pl
from jax.experimental.pallas import tpu as pltpu
from jax.sharding import PartitionSpec as P


def plain(tokens, grad_out, router_weight, expert_index, w_gate, w_up, w_down):
    tok_rows, width = tokens.shape
    top = expert_index.shape[1]
    experts = router_weight.shape[1]
    me = lax.axis_index("expert")
    n = lax.axis_size("expert")
    index_all = lax.all_gather(expert_index, "expert", axis=0, tiled=True)
    tok_all = lax.all_gather(tokens, "expert", axis=0, tiled=True)
    grad_all = lax.all_gather(grad_out, "expert", axis=0, tiled=True)
    gate_in = jnp.dot(tok_all, w_gate[0], preferred_element_type=jnp.float32)
    up_in = jnp.dot(tok_all, w_up[0], preferred_element_type=jnp.float32)
    hidden = jax.nn.silu(gate_in) * up_in
    back = lax.dot_general(
        grad_all, w_down[0], (((1,), (1,)), ((), ())), preferred_element_type=jnp.float32
    )
    dots = jnp.sum(hidden * back, axis=1)
    dots_all = lax.all_gather(dots, "expert", axis=0).T
    labels = jnp.arange(experts, dtype=jnp.int32)
    picked = jnp.any(index_all[:, :, None] == labels, axis=1)
    logits = jnp.dot(tok_all, router_weight, preferred_element_type=jnp.float32)
    weights = jnp.where(picked, jnp.exp(jnp.where(picked, logits, 0.0)), 0.0)
    gates = weights / jnp.sum(weights, axis=1, keepdims=True)
    kept = jnp.where(picked, dots_all, 0.0)
    dense = gates * (kept - jnp.sum(gates * kept, axis=1, keepdims=True))
    cols = width // n
    mine = lax.dynamic_slice_in_dim(tok_all, me * cols, cols, axis=1)
    high = dense.astype(jnp.bfloat16)
    low = (dense - high.astype(jnp.float32)).astype(jnp.bfloat16)
    both = jnp.concatenate([high, low], axis=1)
    part = lax.dot_general(
        mine, both, (((0,), (0,)), ((), ())), preferred_element_type=jnp.float32
    )
    router_grad = lax.psum(part[:, :experts] + part[:, experts:], "dp")
    own = lax.dynamic_slice_in_dim(dots_all, me * tok_rows, tok_rows, axis=0)
    hits = (expert_index[:, :, None] == labels).astype(jnp.float32)
    gate_grad = jnp.sum(hits * own[:, None, :], axis=2)
    return (gate_grad, router_grad)


def layer_kernel(n, dp, tok_in, grad_in, rw_in, idx_in, wg_in, wu_in, wd_in, gg_out, rg_out,
                 tok, grad, rw, idx, wg, wu, wd, hid, eo, lg, dots, part,
                 s_t, r_t, s_a, r_a, s_c, r_c, s_i, r_i, s_d, r_d, s_w, r_w, s_p, r_p, loc):
    plane = n // 2
    line = plane // 2
    me = lax.axis_index("expert")
    xd = lax.axis_index("dp")
    c = me % 2
    q = me // 2
    y = q % 2
    z = q // 2
    rows, width = tok_in.shape
    ff = wg_in.shape[2]
    experts, top = rw_in.shape[0], idx_in.shape[0]
    cut = rows * 5 // 8
    pair = 2 * rows

    def dev(zz, yy, cc):
        return {"expert": (zz * 2 + yy) * 2 + cc}

    def remote(src, dst, ss, rs, where):
        return pltpu.make_async_remote_copy(
            src_ref=src, dst_ref=dst, send_sem=ss, recv_sem=rs,
            device_id=where, device_id_type=pl.DeviceIdType.MESH)

    DOWN, UP, SIDE = 0, 1, 2

    def target(way):
        if way == DOWN:
            return dev(z - 1, y, c)
        if way == UP:
            return dev(z + 1, y, c)
        return dev(z, 1 - y, c)

    kinds = {"t": (tok, tok_in, 0, rows, s_t, r_t),
             "a": (grad, grad_in, 0, cut, s_a, r_a),
             "c": (grad, grad_in, cut, rows - cut, s_c, r_c)}

    def piece(kind, zb, yb, way, own=False):
        buf, inp, lo, size, ss, rs = kinds[kind]
        at = buf.at[zb, pl.ds(pl.multiple_of(yb * rows + lo, 16), size)]
        src = inp.at[pl.ds(lo, size)] if own else at
        return remote(src, at, ss.at[zb * 2 + yb, way], rs.at[zb * 2 + yb], target(way))

    def arrived(kind, zb, yb):
        piece(kind, zb, yb, SIDE).wait_recv()

    barrier = pltpu.get_barrier_semaphore()

    def plane_dev(k):
        return {"expert": ((q + k) % plane) * 2 + c}

    def owner_dev(k):
        return {"dp": (xd + k // 2) % dp, "expert": q * 2 + (c + k) % 2}

    def greet(where):
        pl.semaphore_signal(barrier, inc=1, device_id=where, device_id_type=pl.DeviceIdType.MESH)

    pl.when(z > 0)(lambda: greet(target(DOWN)))
    pl.when(z < line - 1)(lambda: greet(target(UP)))
    greet(target(SIDE))
    for k in range(1, 2 * dp):
        pl.semaphore_signal(barrier, inc=1, device_id=owner_dev(k), device_id_type=pl.DeviceIdType.MESH)
    mine = pl.ds(pl.multiple_of(y * rows, 16), rows)
    local = [pltpu.make_async_copy(tok_in, tok.at[z, mine], loc.at[0]),
             pltpu.make_async_copy(grad_in, grad.at[z, mine], loc.at[1]),
             pltpu.make_async_copy(idx_in, idx.at[q], loc.at[2]),
             pltpu.make_async_copy(wg_in.at[0], wg.at[c], loc.at[3]),
             pltpu.make_async_copy(wu_in.at[0], wu.at[c], loc.at[4]),
             pltpu.make_async_copy(wd_in.at[0], wd.at[c], loc.at[5]),
             pltpu.make_async_copy(rw_in, rw, loc.at[6])]
    for copy in local:
        copy.start()
    pl.when((z > 0) & (z < line - 1))(lambda: pl.semaphore_wait(barrier, 2 + 2 * dp))
    pl.when((z == 0) | (z == line - 1))(lambda: pl.semaphore_wait(barrier, 1 + 2 * dp))

    def own_z(kind, way):
        piece(kind, z, y, way, own=True).start()

    pl.when(z > 0)(lambda: own_z("t", DOWN))
    pl.when(z < line - 1)(lambda: own_z("t", UP))
    own_z("t", SIDE)
    other = {"expert": q * 2 + (1 - c)}
    weights = [remote(wg_in.at[0], wg.at[c], s_w.at[0], r_w.at[0], other),
               remote(wu_in.at[0], wu.at[c], s_w.at[1], r_w.at[1], other),
               remote(wd_in.at[0], wd.at[c], s_w.at[2], r_w.at[2], other)]
    for w in weights:
        w.start()
    index_sends = [remote(idx_in, idx.at[q], s_i.at[k], r_i.at[k], plane_dev(k)) for k in range(1, plane)]
    pl.when(z > 0)(lambda: own_z("a", DOWN))
    pl.when(z < line - 1)(lambda: own_z("a", UP))
    own_z("c", SIDE)

    def relay(kind, s):
        @pl.when(z + s < line)
        def _():
            arrived(kind, z + s, y)

            @pl.when(z > 0)
            def _():
                piece(kind, z + s, y, DOWN).start()
            piece(kind, z + s, y, SIDE).start()

        @pl.when(z - s >= 0)
        def _():
            arrived(kind, z - s, y)

            @pl.when(z < line - 1)
            def _():
                piece(kind, z - s, y, UP).start()
            piece(kind, z - s, y, SIDE).start()

    ft = ff // 3 if ff % 384 == 0 else ff
    dt = width // 4 if width % 512 == 0 else width

    def produce(zp):
        @pl.loop(0, 2)
        def _(r):
            @pl.loop(0, ff // ft)
            def _(j):
                at = pl.ds(pl.multiple_of(j * ft, 128), ft)
                x = tok[zp]
                g = jnp.dot(x, wg[r, :, at], preferred_element_type=jnp.float32)
                u = jnp.dot(x, wu[r, :, at], preferred_element_type=jnp.float32)
                hid[:, at] = (g / (1.0 + jnp.exp(-g)) * u).astype(jnp.bfloat16)

            @pl.loop(0, width // dt)
            def _(j):
                at = pl.ds(pl.multiple_of(j * dt, 128), dt)
                eo[zp, r, :, at] = jnp.dot(
                    hid[...], wd[r, :, at], preferred_element_type=jnp.float32).astype(jnp.bfloat16)
        lg[:, pl.ds(pl.multiple_of(zp * pair, 128), pair)] = lax.dot_general(
            rw[...], tok[zp], (((1,), (1,)), ((), ())), preferred_element_type=jnp.float32)

    def produce_ring(s):
        if s == 0:
            arrived("t", z, 1 - y)
            produce(z)
            return

        @pl.when(z + s < line)
        def _():
            arrived("t", z + s, 1 - y)
            produce(z + s)

        @pl.when(z - s >= 0)
        def _():
            arrived("t", z - s, 1 - y)
            produce(z - s)

    relay("t", 1)
    for copy in local:
        copy.wait()
    for w in weights:
        w.wait_recv()
    produce_ring(0)
    for s in range(2, line):
        relay("t", s)
    own_z("a", SIDE)
    arrived("c", z, 1 - y)
    for yb in range(2):
        pl.when(z > 0)(lambda yb=yb: piece("c", z, yb, DOWN).start())
        pl.when(z < line - 1)(lambda yb=yb: piece("c", z, yb, UP).start())

    for s in range(1, line):
        relay("a", s)
        produce_ring(s)

    for w in index_sends:
        w.start()

    def reduce_pair(zp):
        @pl.loop(0, 2)
        def _(r):
            total = jnp.zeros((pair, 128), jnp.float32)
            for j in range(width // 128):
                at = pl.ds(j * 128, 128)
                total += eo[zp, r, :, at].astype(jnp.float32) * grad[zp, :, at].astype(jnp.float32)
            row = jnp.sum(total.T, axis=0, keepdims=True)
            dots[q, pl.ds(r, 1), pl.ds(pl.multiple_of(zp * pair, 128), pair)] = row

    arrived("a", z, 1 - y)
    reduce_pair(z)
    for s in range(1, line):
        def take(zb, way, ok):
            for yb in range(2):
                arrived("c", zb, yb)
                pl.when(ok)(lambda yb=yb: piece("c", zb, yb, way).start())

        pl.when(z + s < line)(lambda: take(z + s, DOWN, z > 0))
        pl.when(z - s >= 0)(lambda: take(z - s, UP, z < line - 1))

        @pl.when(z + s < line)
        def _():
            arrived("a", z + s, 1 - y)
            reduce_pair(z + s)

        @pl.when(z - s >= 0)
        def _():
            arrived("a", z - s, 1 - y)
            reduce_pair(z - s)

    dot_sends = [remote(dots.at[q], dots.at[q], s_d.at[k], r_d.at[k], plane_dev(k)) for k in range(1, plane)]
    for w in dot_sends:
        w.start()
    for w in index_sends:
        w.wait()
    labels = lax.broadcasted_iota(jnp.int32, (experts, plane * rows), 0)
    chosen = jnp.zeros((experts, plane * rows), jnp.float32)
    for k in range(top):
        named = jnp.concatenate([idx[b, pl.ds(k, 1), :] for b in range(plane)], axis=1)
        chosen = jnp.where(labels == named, 1.0, chosen)
    weight = jnp.where(chosen > 0.0, jnp.exp(jnp.where(chosen > 0.0, lg[...], 0.0)), 0.0)
    gates = weight / jnp.sum(weight, axis=0, keepdims=True)
    for w in dot_sends:
        w.wait()
    all_dots = jnp.concatenate([dots[b] for b in range(plane)], axis=0)
    kept = jnp.where(chosen > 0.0, all_dots, 0.0)
    dense = gates * (kept - jnp.sum(gates * kept, axis=0, keepdims=True))
    high = dense.astype(jnp.bfloat16)
    low = (dense - high.astype(jnp.float32)).astype(jnp.bfloat16)
    cols = width // n
    at = pl.ds(pl.multiple_of(q * 2 * cols, 128), 2 * cols)
    both = jnp.concatenate([high, low], axis=0)
    split = jnp.zeros((2 * experts, 2 * cols), jnp.float32)
    for b in range(line):
        split += jnp.dot(both[:, b * pair:(b + 1) * pair], tok[b, :, at], preferred_element_type=jnp.float32)
    terms = split[:experts] + split[experts:]
    part[0, 0] = terms[:, :cols]
    part[0, 1] = terms[:, cols:]
    part_sends = [remote(part.at[0, (c + k) % 2], part.at[k, 0], s_p.at[k], r_p.at[k], owner_dev(k))
                  for k in range(1, 2 * dp)]
    for w in part_sends:
        w.start()
    own = jnp.concatenate(
        [dots[b, :, pl.ds(pl.multiple_of(q * rows, 128), rows)] for b in range(plane)], axis=0)
    names = idx[q]
    small = lax.broadcasted_iota(jnp.int32, (experts, rows), 0)
    for k in range(top):
        gg_out[pl.ds(k, 1), :] = jnp.sum(
            jnp.where(small == names[k:k + 1, :], own, 0.0), axis=0, keepdims=True)
    for w in part_sends:
        w.wait()
    total = part[0, c]
    for k in range(1, 2 * dp):
        total += part[k, 0]
    rg_out[...] = total

    for w in weights:
        w.wait_send()

    def gone(kind, zb, yb, way):
        piece(kind, zb, yb, way).wait_send()

    for kind in ("t", "a"):
        for zb in range(line):
            pl.when((zb >= z) & (z > 0))(lambda: gone(kind, zb, y, DOWN))
            pl.when((zb <= z) & (z < line - 1))(lambda: gone(kind, zb, y, UP))
            gone(kind, zb, y, SIDE)
    gone("c", z, y, SIDE)
    for zb in range(line):
        for yb in range(2):
            pl.when((zb >= z) & (z > 0))(lambda: gone("c", zb, yb, DOWN))
            pl.when((zb <= z) & (z < line - 1))(lambda: gone("c", zb, yb, UP))


def fused(n, dp, tokens, grad_out, router_weight, expert_index, w_gate, w_up, w_down):
    rows, width = tokens.shape
    ff = w_gate.shape[2]
    top = expert_index.shape[1]
    experts = router_weight.shape[1]
    plane, cols = n // 2, width // n
    line = plane // 2
    pair = 2 * rows
    anywhere = pl.BlockSpec(memory_space=pl.ANY)
    vmem = pl.BlockSpec(memory_space=pltpu.VMEM)
    dma = pltpu.SemaphoreType.DMA
    bf, f32 = jnp.bfloat16, jnp.float32
    gg, rg = pl.pallas_call(
        functools.partial(layer_kernel, n, dp),
        out_shape=(pltpu.VMEM((top, rows), f32), pltpu.VMEM((experts, cols), f32)),
        in_specs=[anywhere] * 7,
        out_specs=(vmem, vmem),
        scratch_shapes=[
            pltpu.VMEM((line, pair, width), bf),
            pltpu.VMEM((line, pair, width), bf),
            pltpu.VMEM((experts, width), bf),
            pltpu.VMEM((plane, top, rows), jnp.int32),
            pltpu.VMEM((2, width, ff), bf),
            pltpu.VMEM((2, width, ff), bf),
            pltpu.VMEM((2, ff, width), bf),
            pltpu.VMEM((pair, ff), bf),
            pltpu.VMEM((line, 2, pair, width), bf),
            pltpu.VMEM((experts, plane * rows), f32),
            pltpu.VMEM((plane, 2, plane * rows), f32),
            pltpu.VMEM((2 * dp, 2, experts, cols), f32),
            dma((plane, 3)), dma((plane,)), dma((plane, 3)), dma((plane,)), dma((plane, 3)), dma((plane,)),
            dma((plane,)), dma((plane,)), dma((plane,)), dma((plane,)),
            dma((3,)), dma((3,)), dma((2 * dp,)), dma((2 * dp,)), dma((7,)),
        ],
        compiler_params=pltpu.CompilerParams(
            collective_id=0, has_side_effects=True, vmem_limit_bytes=60 * 2**20),
    )(tokens, grad_out, router_weight.T, expert_index.T, w_gate, w_up, w_down)
    def finish(a, b, x, y):
        x[...] = a[...]
        y[...] = b[...]
    gg = pltpu.with_memory_space_constraint(gg, pltpu.VMEM)
    rg = pltpu.with_memory_space_constraint(rg, pltpu.VMEM)
    gg, rg = pl.pallas_call(
        finish,
        out_shape=(jax.ShapeDtypeStruct((top, rows), f32), jax.ShapeDtypeStruct((experts, cols), f32)),
        in_specs=[vmem, vmem],
        out_specs=(vmem, vmem),
    )(gg, rg)
    return gg.T, rg.T


def solution(mesh):
    n, dp = mesh.shape["expert"], mesh.shape["dp"]

    def on_device(tokens, grad_out, router_weight, expert_index, w_gate, w_up, w_down):
        rows, width = tokens.shape
        ff = w_gate.shape[2]
        held = 2 * (2 * n // 2 * rows * width * 2 + 6 * ff * width)
        fits = n % 4 == 0 and n >= 8 and held < 44 * 2**20 and width % (128 * n) == 0
        fits = fits and rows % 128 == 0 and router_weight.shape[1] == n
        body = functools.partial(fused, n, dp) if fits else plain
        return body(tokens, grad_out, router_weight, expert_index, w_gate, w_up, w_down)

    in_specs = (
        P(("dp", "expert"), None),
        P(("dp", "expert"), None),
        P(),
        P(("dp", "expert"), None),
        P("expert", None, None),
        P("expert", None, None),
        P("expert", None, None),
    )
    out_specs = (P(("dp", "expert"), None), P("expert", None))
    return jax.shard_map(
        on_device, mesh=mesh, in_specs=in_specs, out_specs=out_specs, check_vma=False
    )
```

```python
import functools

import jax
import jax.numpy as jnp
from jax import lax
from jax.experimental import pallas as pl
from jax.experimental.pallas import tpu as pltpu
from jax.sharding import PartitionSpec as P


def plain(tokens, grad_out, router_weight, expert_index, w_gate, w_up, w_down):
    tok_rows, width = tokens.shape
    top = expert_index.shape[1]
    experts = router_weight.shape[1]
    me = lax.axis_index("expert")
    n = lax.axis_size("expert")
    index_all = lax.all_gather(expert_index, "expert", axis=0, tiled=True)
    tok_all = lax.all_gather(tokens, "expert", axis=0, tiled=True)
    grad_all = lax.all_gather(grad_out, "expert", axis=0, tiled=True)
    gate_in = jnp.dot(tok_all, w_gate[0], preferred_element_type=jnp.float32)
    up_in = jnp.dot(tok_all, w_up[0], preferred_element_type=jnp.float32)
    hidden = jax.nn.silu(gate_in) * up_in
    back = lax.dot_general(
        grad_all, w_down[0], (((1,), (1,)), ((), ())), preferred_element_type=jnp.float32
    )
    dots = jnp.sum(hidden * back, axis=1)
    dots_all = lax.all_gather(dots, "expert", axis=0).T
    labels = jnp.arange(experts, dtype=jnp.int32)
    picked = jnp.any(index_all[:, :, None] == labels, axis=1)
    logits = jnp.dot(tok_all, router_weight, preferred_element_type=jnp.float32)
    weights = jnp.where(picked, jnp.exp(jnp.where(picked, logits, 0.0)), 0.0)
    gates = weights / jnp.sum(weights, axis=1, keepdims=True)
    kept = jnp.where(picked, dots_all, 0.0)
    dense = gates * (kept - jnp.sum(gates * kept, axis=1, keepdims=True))
    cols = width // n
    mine = lax.dynamic_slice_in_dim(tok_all, me * cols, cols, axis=1)
    high = dense.astype(jnp.bfloat16)
    low = (dense - high.astype(jnp.float32)).astype(jnp.bfloat16)
    both = jnp.concatenate([high, low], axis=1)
    part = lax.dot_general(
        mine, both, (((0,), (0,)), ((), ())), preferred_element_type=jnp.float32
    )
    router_grad = lax.psum(part[:, :experts] + part[:, experts:], "dp")
    own = lax.dynamic_slice_in_dim(dots_all, me * tok_rows, tok_rows, axis=0)
    hits = (expert_index[:, :, None] == labels).astype(jnp.float32)
    gate_grad = jnp.sum(hits * own[:, None, :], axis=2)
    return (gate_grad, router_grad)


OUT, IN, SIDE = 0, 1, 2

END = {
    "start": [("S", "x", 3, 0, 0, IN, SIDE), ("S", "x", 3, 0, 1, IN, SIDE),
              ("S", "g", 3, 0, 0, IN), ("S", "g", 3, 0, 1, IN), ("send_down",)],
    "p0": [("F", "x", 2, 0, 0, SIDE), ("F", "x", 2, 0, 1, SIDE), ("W", "x", 3, 1, 0), ("W", "x", 3, 1, 1)],
    "p1": [("F", "x", 1, 0, 0, SIDE)],
    "p2": [("send_hidden",), ("F", "x", 1, 0, 1, SIDE), ("W", "x", 2, 1, 0), ("W", "x", 2, 1, 1)],
    "p3": [("F", "x", 0, 0, 0, SIDE)],
    "p4": [("F", "x", 0, 0, 1, SIDE), ("W", "x", 1, 1, 0), ("W", "x", 1, 1, 1)],
    "p5": [("F", "g", 2, 0, 1, SIDE)],
    "p6": [("F", "g", 1, 0, 0, SIDE), ("W", "x", 0, 1, 0), ("W", "x", 0, 1, 1)],
    "p7": [],
    "r0": [("F", "g", 1, 0, 1, SIDE)],
    "r1": [("F", "g", 0, 0, 0, SIDE)],
    "r2": [("F", "g", 0, 0, 1, SIDE)],
    "r3": [("W", "g", 1, 1, 0), ("W", "g", 1, 1, 1)],
    "r4": [("W", "g", 2, 0, 0)],
    "r5": [("W", "g", 2, 1, 1), ("W", "g", 2, 1, 0)],
    "r6": [("W", "g", 0, 1, 0), ("W", "g", 0, 1, 1)],
    "r7": [],
}
NEXT = {
    "start": [("S", "x", 2, 0, 0, OUT, IN, SIDE), ("S", "x", 2, 0, 1, OUT, IN, SIDE)],
    "p0": [("F", "x", 3, 0, 0, IN, SIDE), ("F", "x", 1, 0, 0, OUT, SIDE),
           ("F", "x", 3, 0, 1, IN, SIDE), ("F", "x", 1, 0, 1, OUT, SIDE),
           ("S", "g", 2, 0, 0, IN, SIDE), ("W", "x", 2, 1, 0), ("W", "x", 2, 1, 1)],
    "p1": [("F", "x", 0, 0, 0, OUT, SIDE), ("F", "g", 3, 0, 0, IN, SIDE)],
    "p2": [("F", "x", 0, 0, 1, OUT, SIDE), ("F", "g", 3, 0, 1, IN, SIDE), ("S", "g", 2, 0, 1, OUT, IN, SIDE),
           ("W", "x", 3, 1, 0), ("W", "x", 3, 1, 1)],
    "p3": [("F", "g", 1, 0, 0, OUT), ("pass_down", 0)],
    "p4": [("W", "x", 1, 1, 0), ("W", "x", 1, 1, 1)],
    "p5": [("pass_down", 1), ("F", "g", 2, 1, 0, IN)],
    "p6": [("F", "g", 1, 0, 1, OUT, SIDE), ("cross_down", 0), ("F", "g", 0, 0, 0, OUT), ("pass_down", 2),
           ("F", "g", 3, 1, 0, IN), ("cross_down", 1), ("F", "g", 0, 0, 1, OUT), ("S", "g", 2, 0, 0, OUT),
           ("P", "g", 2, 1, 0, OUT), ("W", "x", 0, 1, 0), ("W", "x", 0, 1, 1)],
    "p7": [("pass_down", 3), ("cross_down", 2)],
    "r0": [("F", "g", 3, 1, 1, IN)],
    "r1": [],
    "r2": [],
    "r3": [("cross_down", 3)],
    "r4": [("help",)],
    "r5": [("W", "g", 0, 1, 0), ("W", "g", 0, 1, 1)],
    "r6": [("W", "g", 2, 1, 1)],
    "r7": [("W", "g", 1, 1, 0), ("W", "g", 1, 1, 1)],
}
BLOCKS = [((3, 0), (2, 0)), ((1, 0), (3, 0)), ((0, 0), (1, 0)), ((1, 1), (0, 0)),
          ((2, 0), (3, 1)), ((2, 1), (0, 1)), ((0, 1), (2, 1)), ((0, 1), (1, 1))]
CHUNKS = 4


def layer_kernel(n, dp, tok_in, grad_in, rw_in, idx_in, wg_in, wu_in, wd_in, gg_out, rg_out,
                 tok, grad, rw, idx, wg, wu, wd, hid, eo, lg, dots, part, far_wd, sent, extra,
                 s_x, r_x, s_g, r_g, s_i, r_i, s_d, r_d, s_w, r_w, s_p, r_p, s_e, r_e,
                 s_f, r_f, s_fx, r_fx, s_fc, r_fc, s_h, r_h, loc):
    plane = n // 2
    line = plane // 2
    me = lax.axis_index("expert")
    xd = lax.axis_index("dp")
    c = me % 2
    q = me // 2
    y = q % 2
    z = q // 2
    rows, width = tok_in.shape
    ff = wg_in.shape[2]
    experts, top = rw_in.shape[0], idx_in.shape[0]
    pair = 2 * rows
    half = rows // 2
    upper = z // (line // 2)
    own = upper * z + (1 - upper) * (line - 1 - z)
    end = own - (line - 2)
    step = 2 * upper - 1

    def real(m):
        return upper * m + (1 - upper) * (line - 1 - m)

    def side(f):
        return y + f - 2 * y * f

    def dev(zz, yy, cc):
        return {"expert": (zz * 2 + yy) * 2 + cc}

    def remote(src, dst, ss, rs, where):
        return pltpu.make_async_remote_copy(
            src_ref=src, dst_ref=dst, send_sem=ss, recv_sem=rs,
            device_id=where, device_id_type=pl.DeviceIdType.MESH)

    def target(way):
        if way == OUT:
            return dev(z + step, y, c)
        if way == IN:
            return dev(z - step, y, c)
        return dev(z, 1 - y, c)

    kinds = {"x": (tok, tok_in, s_x, r_x), "g": (grad, grad_in, s_g, r_g)}

    def piece(kind, m, f, part_of, way, mine=False):
        buf, inp, ss, rs = kinds[kind]
        zb, yb = real(m), side(f)
        at = buf.at[zb, pl.ds(pl.multiple_of(yb * rows + part_of * half, 16), half)]
        src = inp.at[pl.ds(part_of * half, half)] if mine else at
        slot = (zb * 2 + yb) * 2 + part_of
        return remote(src, at, ss.at[slot, way], rs.at[slot], target(way))

    twin = {"dp": (xd + 1) % dp}
    mate = {"expert": q * 2 + (1 - c)}

    def down_rows(which, k):
        size = ff // dp // CHUNKS
        return pl.ds(pl.multiple_of(which * (ff // dp) + k * size, 16), size)

    def down(k):
        at = down_rows(xd, k)
        return remote(wd_in.at[0, at], far_wd.at[c, at], s_f.at[k], r_f.at[k], target(IN))

    def down_twin(k):
        at = far_wd.at[c, down_rows(xd, k)]
        return remote(at, at, s_fx.at[k], r_fx.at[k], twin)

    def down_mate(other, k):
        at = far_wd.at[c, down_rows((xd + other) % dp, k)]
        return remote(at, at, s_fc.at[other * CHUNKS + k], r_fc.at[other * CHUNKS + k], mate)

    def hidden_send():
        return remote(sent, sent, s_h.at[0], r_h.at[0], target(IN))

    def plane_dev(k):
        return {"expert": ((q + k) % plane) * 2 + c}

    def owner_dev(k):
        return {"dp": (xd + k // 2) % dp, "expert": q * 2 + (c + k) % 2}

    at_end = real(line - 1) * 2 + y
    extra_sends = [remote(extra.at[at_end], extra.at[at_end], s_e.at[k], r_e.at[at_end], plane_dev(k))
                   for k in range(1, plane)]

    def block_dots(left, right):
        total = jnp.zeros((rows, 128), jnp.float32)
        for j in range(width // 128):
            total += left(j).astype(jnp.float32) * right(j).astype(jnp.float32)
        return jnp.sum(total.T, axis=0, keepdims=True)

    dt = width // 4 if width % 512 == 0 else width

    def help_end():
        hidden_send().wait_recv()
        for k in range(CHUNKS):
            down_mate(0, k).wait_recv()
            down_mate(1, k).wait_recv()
        theirs = pl.ds(pl.multiple_of((1 - y) * rows, 16), rows)

        @pl.loop(0, 2)
        def _(r):
            total = jnp.zeros((rows, 128), jnp.float32)
            for j in range(width // dt):
                got = jnp.dot(sent[r], far_wd[r, :, j * dt:(j + 1) * dt],
                              preferred_element_type=jnp.float32).astype(jnp.bfloat16).astype(jnp.float32)
                for i in range(dt // 128):
                    lo = j * dt + i * 128
                    total += got[:, i * 128:(i + 1) * 128] * grad[
                        real(line - 1), theirs, lo:lo + 128].astype(jnp.float32)
            extra[at_end, pl.ds(r, 1), :] = jnp.sum(total.T, axis=0, keepdims=True)
        for w in extra_sends:
            w.start()

    def run(ops):
        for op in ops:
            if op[0] == "send_down":
                for k in range(CHUNKS):
                    down(k).start()
            elif op[0] == "send_hidden":
                hidden_send().start()
            elif op[0] == "pass_down":
                down(op[1]).wait_recv()
                down_twin(op[1]).start()
                down_mate(0, op[1]).start()
            elif op[0] == "cross_down":
                down_twin(op[1]).wait_recv()
                down_mate(1, op[1]).start()
            elif op[0] == "help":
                help_end()
            else:
                what, kind, m, f, part_of = op[:5]
                if what in "FW":
                    piece(kind, m, f, part_of, SIDE).wait_recv()
                for way in op[5:]:
                    piece(kind, m, f, part_of, way, mine=what == "S").start()

    def slot(name):
        if END[name]:
            pl.when(end == 1)(lambda: run(END[name]))
        if NEXT[name]:
            pl.when(end == 0)(lambda: run(NEXT[name]))

    def sent_all(table):
        for ops in table.values():
            for op in ops:
                if op[0] == "send_down":
                    for k in range(CHUNKS):
                        down(k).wait_send()
                elif op[0] == "send_hidden":
                    hidden_send().wait_send()
                elif op[0] == "pass_down":
                    down_twin(op[1]).wait_send()
                    down_mate(0, op[1]).wait_send()
                elif op[0] == "cross_down":
                    down_mate(1, op[1]).wait_send()
                elif op[0] == "help":
                    for w in extra_sends:
                        w.wait_send()
                else:
                    for way in op[5:]:
                        piece(op[1], op[2], op[3], op[4], way).wait_send()

    barrier = pltpu.get_barrier_semaphore()

    def greet(where):
        pl.semaphore_signal(barrier, inc=1, device_id=where, device_id_type=pl.DeviceIdType.MESH)

    pl.when(end == 0)(lambda: greet(target(OUT)))
    greet(target(IN))
    greet(target(SIDE))
    for k in range(1, 2 * dp):
        greet(owner_dev(k))
    mine = pl.ds(pl.multiple_of(y * rows, 16), rows)
    local = [pltpu.make_async_copy(tok_in, tok.at[z, mine], loc.at[0]),
             pltpu.make_async_copy(grad_in, grad.at[z, mine], loc.at[1]),
             pltpu.make_async_copy(idx_in, idx.at[q], loc.at[2]),
             pltpu.make_async_copy(wg_in.at[0], wg.at[c], loc.at[3]),
             pltpu.make_async_copy(wu_in.at[0], wu.at[c], loc.at[4]),
             pltpu.make_async_copy(wd_in.at[0], wd.at[c], loc.at[5]),
             pltpu.make_async_copy(rw_in, rw, loc.at[6])]
    for copy in local:
        copy.start()
    pl.when(end == 0)(lambda: pl.semaphore_wait(barrier, 2 + 2 * dp))
    pl.when(end == 1)(lambda: pl.semaphore_wait(barrier, 1 + 2 * dp))

    slot("start")
    weights = [remote(wg_in.at[0], wg.at[c], s_w.at[0], r_w.at[0], mate),
               remote(wu_in.at[0], wu.at[c], s_w.at[1], r_w.at[1], mate),
               remote(wd_in.at[0], wd.at[c], s_w.at[2], r_w.at[2], mate)]
    for w in weights:
        w.start()
    index_sends = [remote(idx_in, idx.at[q], s_i.at[k], r_i.at[k], plane_dev(k)) for k in range(1, plane)]

    ft = ff // 3 if ff % 384 == 0 else ff

    def produce(zp, r, first, keep):
        @pl.loop(0, ff // ft)
        def _(j):
            at = pl.ds(pl.multiple_of(j * ft, 128), ft)
            x = tok[zp]
            g = jnp.dot(x, wg[r, :, at], preferred_element_type=jnp.float32)
            u = jnp.dot(x, wu[r, :, at], preferred_element_type=jnp.float32)
            hid[:, at] = (g / (1.0 + jnp.exp(-g)) * u).astype(jnp.bfloat16)

        if keep:
            @pl.when(end == 1)
            def _():
                sent[r] = hid[pl.ds(pl.multiple_of((1 - y) * rows, 16), rows), :]

        @pl.loop(0, width // dt)
        def _(j):
            at = pl.ds(pl.multiple_of(j * dt, 128), dt)
            eo[zp, r, :, at] = jnp.dot(
                hid[...], wd[r, :, at], preferred_element_type=jnp.float32).astype(jnp.bfloat16)
        if first:
            lg[:, pl.ds(pl.multiple_of(zp * pair, 128), pair)] = lax.dot_general(
                rw[...], tok[zp], (((1,), (1,)), ((), ())), preferred_element_type=jnp.float32)

    order = [2 + end, 3 - end, 1, 0]
    for i in range(line):
        for k in range(2):
            slot("p" + str(2 * i + k))
            if i == 0 and k == 0:
                for copy in local:
                    copy.wait()
            if i == 0 and k == 1:
                for w in weights:
                    w.wait_recv()
            produce(real(order[i]), c + k - 2 * c * k, k == 0, i == 0)

    for w in index_sends:
        w.start()

    def reduce_block(zb, yb):
        at = pl.ds(pl.multiple_of(yb * rows, 16), rows)

        @pl.loop(0, 2)
        def _(r):
            row = block_dots(lambda j: eo[zb, r, at, j * 128:(j + 1) * 128],
                             lambda j: grad[zb, at, j * 128:(j + 1) * 128])
            dots[q, zb * 2 + yb, pl.ds(r, 1), :] = row

    for i, (a, b) in enumerate(BLOCKS):
        slot("r" + str(i))
        m = end * a[0] + (1 - end) * b[0]
        f = end * a[1] + (1 - end) * b[1]
        if i < len(BLOCKS) - 1:
            reduce_block(real(m), side(f))
        else:
            pl.when(end == 0)(lambda: reduce_block(real(m), side(f)))

    dot_sends = [remote(dots.at[q], dots.at[q], s_d.at[k], r_d.at[k], plane_dev(k)) for k in range(1, plane)]
    for w in dot_sends:
        w.start()
    for w in index_sends:
        w.wait()
    labels = lax.broadcasted_iota(jnp.int32, (experts, plane * rows), 0)
    chosen = jnp.zeros((experts, plane * rows), jnp.float32)
    for k in range(top):
        named = jnp.concatenate([idx[b, pl.ds(k, 1), :] for b in range(plane)], axis=1)
        chosen = jnp.where(labels == named, 1.0, chosen)
    weight = jnp.where(chosen > 0.0, jnp.exp(jnp.where(chosen > 0.0, lg[...], 0.0)), 0.0)
    gates = weight / jnp.sum(weight, axis=0, keepdims=True)
    ends = {0: 2, 1: 3, plane - 2: plane - 4, plane - 1: plane - 3}
    for b, helper in ends.items():
        pl.when(q != helper)(lambda: remote(
            extra.at[b], extra.at[b], s_e.at[1], r_e.at[b], plane_dev(1)).wait_recv())
    for w in dot_sends:
        w.wait()

    def dots_of(b):
        blocks = [dots[b, k] for k in range(plane)]
        if b in ends:
            blocks[b ^ 1] = extra[b]
        return jnp.concatenate(blocks, axis=1)

    all_dots = jnp.concatenate([dots_of(b) for b in range(plane)], axis=0)
    kept = jnp.where(chosen > 0.0, all_dots, 0.0)
    dense = gates * (kept - jnp.sum(gates * kept, axis=0, keepdims=True))
    high = dense.astype(jnp.bfloat16)
    low = (dense - high.astype(jnp.float32)).astype(jnp.bfloat16)
    cols = width // n
    at = pl.ds(pl.multiple_of(q * 2 * cols, 128), 2 * cols)
    both = jnp.concatenate([high, low], axis=0)
    split = jnp.zeros((2 * experts, 2 * cols), jnp.float32)
    for b in range(line):
        split += jnp.dot(both[:, b * pair:(b + 1) * pair], tok[b, :, at], preferred_element_type=jnp.float32)
    terms = split[:experts] + split[experts:]
    part[0, 0] = terms[:, :cols]
    part[0, 1] = terms[:, cols:]
    part_sends = [remote(part.at[0, (c + k) % 2], part.at[k, 0], s_p.at[k], r_p.at[k], owner_dev(k))
                  for k in range(1, 2 * dp)]
    for w in part_sends:
        w.start()
    held = [jnp.where(q == (b ^ 1), extra[b], dots[b, q]) if b in ends else dots[b, q] for b in range(plane)]
    held = jnp.concatenate(held, axis=0)
    names = idx[q]
    small = lax.broadcasted_iota(jnp.int32, (experts, rows), 0)
    for k in range(top):
        gg_out[pl.ds(k, 1), :] = jnp.sum(
            jnp.where(small == names[k:k + 1, :], held, 0.0), axis=0, keepdims=True)
    for w in weights:
        w.wait_send()
    pl.when(end == 1)(lambda: sent_all(END))
    pl.when(end == 0)(lambda: sent_all(NEXT))
    for w in part_sends:
        w.wait()
    total = part[0, c]
    for k in range(1, 2 * dp):
        total += part[k, 0]
    rg_out[...] = total


def fused(n, dp, tokens, grad_out, router_weight, expert_index, w_gate, w_up, w_down):
    rows, width = tokens.shape
    ff = w_gate.shape[2]
    top = expert_index.shape[1]
    experts = router_weight.shape[1]
    plane, cols = n // 2, width // n
    line = plane // 2
    pair = 2 * rows
    anywhere = pl.BlockSpec(memory_space=pl.ANY)
    vmem = pl.BlockSpec(memory_space=pltpu.VMEM)
    dma = pltpu.SemaphoreType.DMA
    bf, f32 = jnp.bfloat16, jnp.float32
    gg, rg = pl.pallas_call(
        functools.partial(layer_kernel, n, dp),
        out_shape=(pltpu.VMEM((top, rows), f32), pltpu.VMEM((experts, cols), f32)),
        in_specs=[anywhere] * 7,
        out_specs=(vmem, vmem),
        scratch_shapes=[
            pltpu.VMEM((line, pair, width), bf),
            pltpu.VMEM((line, pair, width), bf),
            pltpu.VMEM((experts, width), bf),
            pltpu.VMEM((plane, top, rows), jnp.int32),
            pltpu.VMEM((2, width, ff), bf),
            pltpu.VMEM((2, width, ff), bf),
            pltpu.VMEM((2, ff, width), bf),
            pltpu.VMEM((pair, ff), bf),
            pltpu.VMEM((line, 2, pair, width), bf),
            pltpu.VMEM((experts, plane * rows), f32),
            pltpu.VMEM((plane, plane, 2, rows), f32),
            pltpu.VMEM((2 * dp, 2, experts, cols), f32),
            pltpu.VMEM((2, ff, width), bf),
            pltpu.VMEM((2, rows, ff), bf),
            pltpu.VMEM((plane, 2, rows), f32),
            dma((2 * plane, 3)), dma((2 * plane,)), dma((2 * plane, 3)), dma((2 * plane,)),
            dma((plane,)), dma((plane,)), dma((plane,)), dma((plane,)),
            dma((3,)), dma((3,)), dma((2 * dp,)), dma((2 * dp,)), dma((plane,)), dma((plane,)),
            dma((CHUNKS,)), dma((CHUNKS,)), dma((CHUNKS,)), dma((CHUNKS,)),
            dma((dp * CHUNKS,)), dma((dp * CHUNKS,)), dma((1,)), dma((1,)), dma((7,)),
        ],
        compiler_params=pltpu.CompilerParams(
            collective_id=0, has_side_effects=True, vmem_limit_bytes=60 * 2**20),
    )(tokens, grad_out, router_weight.T, expert_index.T, w_gate, w_up, w_down)
    def finish(a, b, x, y):
        x[...] = a[...]
        y[...] = b[...]
    gg = pltpu.with_memory_space_constraint(gg, pltpu.VMEM)
    rg = pltpu.with_memory_space_constraint(rg, pltpu.VMEM)
    gg, rg = pl.pallas_call(
        finish,
        out_shape=(jax.ShapeDtypeStruct((top, rows), f32), jax.ShapeDtypeStruct((experts, cols), f32)),
        in_specs=[vmem, vmem],
        out_specs=(vmem, vmem),
    )(gg, rg)
    return gg.T, rg.T


def solution(mesh):
    n, dp = mesh.shape["expert"], mesh.shape["dp"]

    def on_device(tokens, grad_out, router_weight, expert_index, w_gate, w_up, w_down):
        rows, width = tokens.shape
        ff = w_gate.shape[2]
        held = 2 * (2 * n // 2 * rows * width * 2 + 8 * ff * width)
        fits = n % 4 == 0 and n // 4 == 4 and dp == 2 and held < 44 * 2**20 and width % (128 * n) == 0
        fits = fits and ff % (16 * dp * CHUNKS) == 0 and ff % 128 == 0
        fits = fits and rows % 128 == 0 and router_weight.shape[1] == n
        body = functools.partial(fused, n, dp) if fits else plain
        return body(tokens, grad_out, router_weight, expert_index, w_gate, w_up, w_down)

    in_specs = (
        P(("dp", "expert"), None),
        P(("dp", "expert"), None),
        P(),
        P(("dp", "expert"), None),
        P("expert", None, None),
        P("expert", None, None),
        P("expert", None, None),
    )
    out_specs = (P(("dp", "expert"), None), P("expert", None))
    return jax.shard_map(
        on_device, mesh=mesh, in_specs=in_specs, out_specs=out_specs, check_vma=False
    )
```

```python
import functools

import jax
import jax.numpy as jnp
from jax import lax
from jax.experimental import pallas as pl
from jax.experimental.pallas import tpu as pltpu
from jax.sharding import PartitionSpec as P


def plain(tokens, grad_out, router_weight, expert_index, w_gate, w_up, w_down):
    tok_rows, width = tokens.shape
    top = expert_index.shape[1]
    experts = router_weight.shape[1]
    me = lax.axis_index("expert")
    n = lax.axis_size("expert")
    index_all = lax.all_gather(expert_index, "expert", axis=0, tiled=True)
    tok_all = lax.all_gather(tokens, "expert", axis=0, tiled=True)
    grad_all = lax.all_gather(grad_out, "expert", axis=0, tiled=True)
    gate_in = jnp.dot(tok_all, w_gate[0], preferred_element_type=jnp.float32)
    up_in = jnp.dot(tok_all, w_up[0], preferred_element_type=jnp.float32)
    hidden = jax.nn.silu(gate_in) * up_in
    back = lax.dot_general(
        grad_all, w_down[0], (((1,), (1,)), ((), ())), preferred_element_type=jnp.float32
    )
    dots = jnp.sum(hidden * back, axis=1)
    dots_all = lax.all_gather(dots, "expert", axis=0).T
    labels = jnp.arange(experts, dtype=jnp.int32)
    picked = jnp.any(index_all[:, :, None] == labels, axis=1)
    logits = jnp.dot(tok_all, router_weight, preferred_element_type=jnp.float32)
    weights = jnp.where(picked, jnp.exp(jnp.where(picked, logits, 0.0)), 0.0)
    gates = weights / jnp.sum(weights, axis=1, keepdims=True)
    kept = jnp.where(picked, dots_all, 0.0)
    dense = gates * (kept - jnp.sum(gates * kept, axis=1, keepdims=True))
    cols = width // n
    mine = lax.dynamic_slice_in_dim(tok_all, me * cols, cols, axis=1)
    high = dense.astype(jnp.bfloat16)
    low = (dense - high.astype(jnp.float32)).astype(jnp.bfloat16)
    both = jnp.concatenate([high, low], axis=1)
    part = lax.dot_general(
        mine, both, (((0,), (0,)), ((), ())), preferred_element_type=jnp.float32
    )
    router_grad = lax.psum(part[:, :experts] + part[:, experts:], "dp")
    own = lax.dynamic_slice_in_dim(dots_all, me * tok_rows, tok_rows, axis=0)
    hits = (expert_index[:, :, None] == labels).astype(jnp.float32)
    gate_grad = jnp.sum(hits * own[:, None, :], axis=2)
    return (gate_grad, router_grad)


OUT, IN, SIDE = 0, 1, 2

END = {
    "start": [("S", "x", 3, 0, 0, IN, SIDE), ("S", "x", 3, 0, 1, IN, SIDE),
              ("S", "g", 3, 0, 0, IN), ("S", "g", 3, 0, 1, IN), ("send_down",)],
    "p0": [("F", "x", 2, 0, 0, SIDE), ("F", "x", 2, 0, 1, SIDE), ("W", "x", 3, 1, 0), ("W", "x", 3, 1, 1)],
    "p1": [("F", "x", 1, 0, 0, SIDE)],
    "p2": [("send_hidden", 0), ("F", "x", 1, 0, 1, SIDE), ("W", "x", 2, 1, 0), ("W", "x", 2, 1, 1)],
    "p3": [("F", "x", 0, 0, 0, SIDE)],
    "p4": [("send_hidden", 1), ("F", "x", 0, 0, 1, SIDE), ("W", "x", 1, 1, 0), ("W", "x", 1, 1, 1)],
    "p5": [("F", "g", 1, 0, 0, SIDE)],
    "r0": [],
    "r1": [("F", "g", 1, 0, 1, SIDE)],
    "p6": [("W", "x", 0, 1, 0), ("W", "x", 0, 1, 1)],
    "p7": [("F", "g", 0, 0, 0, SIDE)],
    "r2": [("F", "g", 0, 0, 1, SIDE)],
    "r3": [("W", "g", 1, 1, 0), ("W", "g", 1, 1, 1)],
    "r4": [("wait_rest",)],
    "r5": [("W", "g", 0, 1, 0), ("W", "g", 0, 1, 1)],
    "r6": [("W", "g", 2, 1, 0), ("W", "g", 2, 1, 1)],
    "r7": [],
    "last": [],
}
NEXT = {
    "start": [("S", "x", 2, 0, 0, OUT, IN, SIDE), ("S", "x", 2, 0, 1, OUT, IN, SIDE)],
    "p0": [("F", "x", 3, 0, 0, IN, SIDE), ("F", "x", 1, 0, 0, OUT, SIDE),
           ("F", "x", 3, 0, 1, IN, SIDE), ("F", "x", 1, 0, 1, OUT, SIDE),
           ("S", "g", 2, 0, 0, IN, SIDE), ("S", "g", 2, 0, 1, IN), ("W", "x", 2, 1, 0), ("W", "x", 2, 1, 1)],
    "p1": [("F", "g", 3, 0, 0, IN, SIDE), ("F", "x", 0, 0, 0, OUT, SIDE)],
    "p2": [("F", "x", 0, 0, 1, OUT), ("send_rest",), ("F", "g", 3, 0, 1, IN, SIDE), ("S", "g", 2, 0, 1, SIDE),
           ("W", "x", 3, 1, 0), ("F", "x", 3, 1, 1, IN), ("F", "g", 1, 0, 0, OUT), ("pass_down", 0)],
    "p3": [("pass_down", 1)],
    "p4": [("W", "x", 1, 1, 0), ("W", "x", 1, 1, 1), ("F", "g", 1, 0, 1, OUT, SIDE)],
    "p5": [("F", "g", 0, 0, 0, OUT), ("F", "g", 2, 1, 0, IN), ("pass_down", 2), ("cross_down", 0)],
    "r0": [("F", "g", 0, 0, 1, OUT), ("P", "g", 2, 1, 0, OUT), ("pass_down", 3), ("cross_down", 1)],
    "r1": [("F", "g", 3, 1, 0, IN)],
    "p6": [("pass_down", 4), ("W", "x", 0, 1, 1), ("W", "x", 0, 1, 0)],
    "p7": [("pass_down", 5), ("cross_down", 2)],
    "r2": [("F", "g", 3, 1, 1, IN), ("cross_down", 3), ("F", "g", 2, 1, 1, OUT)],
    "r3": [("cross_down", 4)],
    "r4": [],
    "r5": [],
    "r6": [("cross_down", 5), ("help", 0), ("W", "g", 0, 1, 0), ("W", "g", 0, 1, 1)],
    "r7": [("W", "g", 1, 1, 0), ("W", "g", 1, 1, 1)],
    "last": [("help", 1)],
}
BLOCKS = [((3, 0), (2, 0)), ((1, 0), (3, 0)), ((0, 0), (1, 0)), ((1, 1), (0, 0)),
          ((2, 0), (3, 1)), ((0, 1), (2, 1)), ((2, 1), (0, 1)), ((2, 1), (1, 1))]
EARLY = 2
CHUNKS = 6
KEPT = 6


def layer_kernel(n, dp, tok_in, grad_in, rw_in, idx_in, wg_in, wu_in, wd_in, gg_out, rg_out,
                 tok, grad, rw, idx, wg, wu, wd, hid, eo, lg, dots, part, far_wd, sent, more,
                 s_way, r_x, r_g, s_i, r_i, s_d, r_d, s_w, r_w, s_p, r_p,
                 s_f, r_f, s_fx, r_fx, s_fc, r_fc, s_h, r_h, s_t, r_t, loc):
    plane = n // 2
    line = plane // 2
    me = lax.axis_index("expert")
    xd = lax.axis_index("dp")
    c = me % 2
    q = me // 2
    y = q % 2
    z = q // 2
    rows, width = tok_in.shape
    ff = wg_in.shape[2]
    experts, top = rw_in.shape[0], idx_in.shape[0]
    pair = 2 * rows
    half = rows // 2
    upper = z // (line // 2)
    own = upper * z + (1 - upper) * (line - 1 - z)
    end = own - (line - 2)
    step = 2 * upper - 1

    def real(m):
        return upper * m + (1 - upper) * (line - 1 - m)

    def side(f):
        return y + f - 2 * y * f

    def dev(zz, yy, cc):
        return {"expert": (zz * 2 + yy) * 2 + cc}

    def remote(src, dst, ss, rs, where):
        return pltpu.make_async_remote_copy(
            src_ref=src, dst_ref=dst, send_sem=ss, recv_sem=rs,
            device_id=where, device_id_type=pl.DeviceIdType.MESH)

    def target(way):
        if way == OUT:
            return dev(z + step, y, c)
        if way == IN:
            return dev(z - step, y, c)
        return dev(z, 1 - y, c)

    kinds = {"x": (tok, r_x), "g": (grad, r_g)}

    def piece(kind, m, f, part_of, way):
        buf, rs = kinds[kind]
        zb, yb = real(m), side(f)
        at = buf.at[zb, pl.ds(pl.multiple_of(yb * rows + part_of * half, 16), half)]
        slot = (zb * 2 + yb) * 2 + part_of
        return remote(at, at, s_way.at[way], rs.at[slot], target(way))

    twin = {"dp": (xd + 1) % dp}
    mate = {"expert": q * 2 + (1 - c)}

    def down_rows(which, k):
        size = ff // dp // CHUNKS
        return pl.ds(pl.multiple_of(which * (ff // dp) + k * size, 16), size)

    def down(k):
        at = down_rows(xd, k)
        return remote(wd_in.at[0, at], far_wd.at[c, at], s_f.at[0], r_f.at[k], target(IN))

    def down_twin(k):
        at = far_wd.at[c, down_rows(xd, k)]
        return remote(at, at, s_fx.at[0], r_fx.at[k], twin)

    def down_mate(other, k):
        at = far_wd.at[c, down_rows((xd + other) % dp, k)]
        return remote(at, at, s_fc.at[0], r_fc.at[0], mate)

    fewer = more.shape[1]
    rest = rows - fewer

    def hidden_send(which, r):
        buf = more if which else sent
        return remote(buf.at[r], buf.at[r], s_h.at[2 * which + r], r_h.at[2 * which + r], target(IN))

    def rest_send(way):
        at = grad.at[real(line - 2), pl.ds(pl.multiple_of(y * rows + fewer, 16), rest)]
        return remote(at, at, s_t.at[0], r_t.at[0], target(way))

    def plane_dev(k):
        return {"expert": ((q + k) % plane) * 2 + c}

    def owner_dev(k):
        return {"dp": (xd + k // 2) % dp, "expert": q * 2 + (c + k) % 2}

    def few(buf, k, ss, rs):
        return remote(buf.at[pl.ds(0, k)], buf.at[pl.ds(0, k)], ss, rs, plane_dev(1))

    def block_dots(left, right):
        total = jnp.zeros((rows, 128), jnp.float32)
        for j in range(width // 128):
            total += left(j).astype(jnp.float32) * right(j).astype(jnp.float32)
        return jnp.sum(total.T, axis=0, keepdims=True)

    dt = width // 4 if width % 512 == 0 else width

    def help_end(which):
        if which == 0:
            remote(far_wd.at[0], far_wd.at[0], s_fc.at[0], r_fc.at[0], mate).wait_recv()
        buf = more if which else sent
        count = buf.shape[1]
        zb, base = (real(line - 2), y * rows) if which else (real(line - 1), (1 - y) * rows)
        theirs = pl.ds(pl.multiple_of(base, 16), count)

        @pl.loop(0, 2)
        def _(r):
            hidden_send(which, r).wait_recv()
            total = jnp.zeros((count, 128), jnp.float32)
            for j in range(width // dt):
                got = jnp.dot(buf[r], far_wd[r, :, j * dt:(j + 1) * dt],
                              preferred_element_type=jnp.float32).astype(jnp.bfloat16).astype(jnp.float32)
                for i in range(dt // 128):
                    lo = j * dt + i * 128
                    total += got[:, i * 128:(i + 1) * 128] * grad[
                        zb, theirs, lo:lo + 128].astype(jnp.float32)
            row = jnp.sum(total.T, axis=0, keepdims=True)
            if count < rows:
                row = jnp.concatenate([row, jnp.zeros((1, rows - count), jnp.float32)], axis=1)
            dots[q, plane + which, pl.ds(r, 1), :] = row

    def run(ops):
        for op in ops:
            if op[0] == "send_down":
                for k in range(CHUNKS):
                    down(k).start()
            elif op[0] == "send_hidden":
                hidden_send(op[1], 0).start()
                hidden_send(op[1], 1).start()
            elif op[0] == "send_rest":
                if rest:
                    rest_send(OUT).start()
            elif op[0] == "wait_rest":
                if rest:
                    rest_send(SIDE).wait_recv()
            elif op[0] == "pass_down":
                down(op[1]).wait_recv()
                down_twin(op[1]).start()
                down_mate(0, op[1]).start()
            elif op[0] == "cross_down":
                down_twin(op[1]).wait_recv()
                down_mate(1, op[1]).start()
            elif op[0] == "help":
                help_end(op[1])
            else:
                what, kind, m, f, part_of = op[:5]
                if what in "FW":
                    piece(kind, m, f, part_of, SIDE).wait_recv()
                for way in op[5:]:
                    piece(kind, m, f, part_of, way).start()

    def slot(name):
        if END[name]:
            pl.when(end == 1)(lambda: run(END[name]))
        if NEXT[name]:
            pl.when(end == 0)(lambda: run(NEXT[name]))

    def sent_all(table):
        ways = [way for ops in table.values() for op in ops if op[0] in ("S", "F", "P") for way in op[5:]]
        for way in range(3):
            if way in ways:
                at = tok.at[:, pl.ds(0, ways.count(way) * half // line)]
                remote(at, at, s_way.at[way], r_x.at[0], target(SIDE)).wait_send()
        if table is END:
            at = far_wd.at[0, pl.ds(0, ff // dp)]
            remote(at, at, s_f.at[0], r_f.at[0], target(IN)).wait_send()
            for k in range(4):
                hidden_send(k // 2, k % 2).wait_send()
            return
        at = far_wd.at[0, pl.ds(0, ff // dp)]
        remote(at, at, s_fx.at[0], r_fx.at[0], twin).wait_send()
        remote(far_wd.at[0], far_wd.at[0], s_fc.at[0], r_fc.at[0], mate).wait_send()
        if rest:
            rest_send(OUT).wait_send()

    barrier = pltpu.get_barrier_semaphore()

    def greet(where):
        pl.semaphore_signal(barrier, inc=1, device_id=where, device_id_type=pl.DeviceIdType.MESH)

    pl.when(end == 0)(lambda: greet(target(OUT)))
    greet(target(IN))
    greet(target(SIDE))
    for k in range(1, 2 * dp):
        greet(owner_dev(k))
    mine = pl.ds(pl.multiple_of(y * rows, 16), rows)
    local = [pltpu.make_async_copy(tok_in, tok.at[z, mine], loc.at[0]),
             pltpu.make_async_copy(grad_in, grad.at[z, mine], loc.at[1]),
             pltpu.make_async_copy(idx_in, idx.at[q], loc.at[2]),
             pltpu.make_async_copy(wg_in.at[0], wg.at[c], loc.at[3]),
             pltpu.make_async_copy(wu_in.at[0], wu.at[c], loc.at[4]),
             pltpu.make_async_copy(wd_in.at[0], wd.at[c], loc.at[5]),
             pltpu.make_async_copy(rw_in, rw, loc.at[6])]
    for copy in local[:2]:
        copy.start()
    pl.when(end == 0)(lambda: pl.semaphore_wait(barrier, 2 + 2 * dp))
    pl.when(end == 1)(lambda: pl.semaphore_wait(barrier, 1 + 2 * dp))

    for copy in local[:2]:
        copy.wait()
    slot("start")
    for copy in local[2:]:
        copy.start()
    weights = [remote(wg_in.at[0], wg.at[c], s_w.at[0], r_w.at[0], mate),
               remote(wu_in.at[0], wu.at[c], s_w.at[1], r_w.at[1], mate),
               remote(wd_in.at[0], wd.at[c], s_w.at[2], r_w.at[2], mate)]
    for w in weights:
        w.start()
    index_sends = [remote(idx_in, idx.at[q], s_i.at[0], r_i.at[0], plane_dev(k)) for k in range(1, plane)]

    ft = ff // 3 if ff % 384 == 0 else ff

    def produce(zp, r, first, keep):
        @pl.loop(0, ff // ft)
        def _(j):
            at = pl.ds(pl.multiple_of(j * ft, 128), ft)
            x = tok[zp]
            g = jnp.dot(x, wg[r, :, at], preferred_element_type=jnp.float32)
            u = jnp.dot(x, wu[r, :, at], preferred_element_type=jnp.float32)
            hid[:, at] = (g / (1.0 + jnp.exp(-g)) * u).astype(jnp.bfloat16)

        if keep == 0:
            @pl.when(end == 1)
            def _():
                sent[r] = hid[pl.ds(pl.multiple_of((1 - y) * rows, 16), rows), :]
        if keep == 1:
            @pl.when(end == 1)
            def _():
                more[r] = hid[pl.ds(pl.multiple_of(y * rows, 16), fewer), :]

        @pl.loop(0, width // dt)
        def _(j):
            at = pl.ds(pl.multiple_of(j * dt, 128), dt)
            eo[zp, r, :, at] = jnp.dot(
                hid[...], wd[r, :, at], preferred_element_type=jnp.float32).astype(jnp.bfloat16)
        if first:
            lg[:, pl.ds(pl.multiple_of(zp * pair, 128), pair)] = lax.dot_general(
                rw[...], tok[zp], (((1,), (1,)), ((), ())), preferred_element_type=jnp.float32)

    def reduce_block(zb, yb):
        at = pl.ds(pl.multiple_of(yb * rows, 16), rows)

        @pl.loop(0, 2)
        def _(r):
            row = block_dots(lambda j: eo[zb, r, at, j * 128:(j + 1) * 128],
                             lambda j: grad[zb, at, j * 128:(j + 1) * 128])
            dots[q, zb * 2 + yb, pl.ds(r, 1), :] = row

    def reduce_some(lo, hi):
        for i in range(lo, hi):
            slot("r" + str(i))
            a, b = BLOCKS[i]
            m = end * a[0] + (1 - end) * b[0]
            f = end * a[1] + (1 - end) * b[1]
            if a != BLOCKS[i - 1][0] and (rest or a != (2, 0)):
                reduce_block(real(m), side(f))
            else:
                pl.when(end == 0)(lambda: reduce_block(real(m), side(f)))

    order = [2 + end, 3 - end, 1, 0]
    for i in range(line):
        if i == line - 1:
            reduce_some(0, EARLY)
        for k in range(2):
            slot("p" + str(2 * i + k))
            if i == 0 and k == 0:
                for copy in local[2:]:
                    copy.wait()
            if i == 0 and k == 1:
                for w in weights:
                    w.wait_recv()
            produce(real(order[i]), c + k - 2 * c * k, k == 0, i)

    for w in index_sends:
        w.start()

    reduce_some(EARLY, len(BLOCKS))
    slot("last")

    dot_sends = [remote(dots.at[q], dots.at[q], s_d.at[0], r_d.at[0], plane_dev(k)) for k in range(1, plane)]
    for w in dot_sends:
        w.start()
    few(idx, plane - 1, s_i.at[0], r_i.at[0]).wait()
    labels = lax.broadcasted_iota(jnp.int32, (experts, plane * rows), 0)
    chosen = jnp.zeros((experts, plane * rows), jnp.float32)
    for k in range(top):
        named = jnp.concatenate([idx[b, pl.ds(k, 1), :] for b in range(plane)], axis=1)
        chosen = jnp.where(labels == named, 1.0, chosen)
    weight = jnp.where(chosen > 0.0, jnp.exp(jnp.where(chosen > 0.0, lg[...], 0.0)), 0.0)
    gates = weight / jnp.sum(weight, axis=0, keepdims=True)
    ends = (0, 1, plane - 2, plane - 1)
    few(dots, plane - 1, s_d.at[0], r_d.at[0]).wait()
    lanes = lax.broadcasted_iota(jnp.int32, (2, rows), 1)

    def next_to(b):
        return b + 2 if b < 2 else b - 2

    def patched(b):
        helped = dots[next_to(b), plane + 1]
        return jnp.where(lanes < fewer, helped, dots[b, next_to(b)]) if rest else helped

    def dots_of(b):
        blocks = [dots[b, k] for k in range(plane)]
        if b in ends:
            blocks[b ^ 1] = dots[next_to(b), plane]
            blocks[next_to(b)] = patched(b)
        return jnp.concatenate(blocks, axis=1)

    all_dots = jnp.concatenate([dots_of(b) for b in range(plane)], axis=0)
    kept = jnp.where(chosen > 0.0, all_dots, 0.0)
    dense = gates * (kept - jnp.sum(gates * kept, axis=0, keepdims=True))
    high = dense.astype(jnp.bfloat16)
    low = (dense - high.astype(jnp.float32)).astype(jnp.bfloat16)
    cols = width // n
    at = pl.ds(pl.multiple_of(q * 2 * cols, 128), 2 * cols)
    both = jnp.concatenate([high, low], axis=0)
    split = jnp.zeros((2 * experts, 2 * cols), jnp.float32)
    for b in range(line):
        split += jnp.dot(both[:, b * pair:(b + 1) * pair], tok[b, :, at], preferred_element_type=jnp.float32)
    terms = split[:experts] + split[experts:]
    part[0, 0] = terms[:, :cols]
    part[0, 1] = terms[:, cols:]
    part_sends = [remote(part.at[0, (c + k) % 2], part.at[k, 0], s_p.at[0], r_p.at[0], owner_dev(k))
                  for k in range(1, 2 * dp)]
    for w in part_sends:
        w.start()
    held = []
    for b in range(plane):
        row = dots[b, q]
        if b in ends:
            row = jnp.where(q == (b ^ 1), dots[next_to(b), plane], jnp.where(q == next_to(b), patched(b), row))
        held.append(row)
    held = jnp.concatenate(held, axis=0)
    names = idx[q]
    small = lax.broadcasted_iota(jnp.int32, (experts, rows), 0)
    for k in range(top):
        gg_out[pl.ds(k, 1), :] = jnp.sum(
            jnp.where(small == names[k:k + 1, :], held, 0.0), axis=0, keepdims=True)
    for w in weights:
        w.wait_send()
    pl.when(end == 1)(lambda: sent_all(END))
    pl.when(end == 0)(lambda: sent_all(NEXT))
    at = part.at[pl.ds(0, 2 * dp - 1), 0]
    remote(at, at, s_p.at[0], r_p.at[0], mate).wait()
    total = part[0, c]
    for k in range(1, 2 * dp):
        total += part[k, 0]
    rg_out[...] = total


def fused(n, dp, tokens, grad_out, router_weight, expert_index, w_gate, w_up, w_down):
    rows, width = tokens.shape
    ff = w_gate.shape[2]
    top = expert_index.shape[1]
    experts = router_weight.shape[1]
    plane, cols = n // 2, width // n
    line = plane // 2
    pair = 2 * rows
    anywhere = pl.BlockSpec(memory_space=pl.ANY)
    vmem = pl.BlockSpec(memory_space=pltpu.VMEM)
    dma = pltpu.SemaphoreType.DMA
    bf, f32 = jnp.bfloat16, jnp.float32
    gg, rg = pl.pallas_call(
        functools.partial(layer_kernel, n, dp),
        out_shape=(pltpu.VMEM((top, rows), f32), pltpu.VMEM((experts, cols), f32)),
        in_specs=[anywhere] * 7,
        out_specs=(vmem, vmem),
        scratch_shapes=[
            pltpu.VMEM((line, pair, width), bf),
            pltpu.VMEM((line, pair, width), bf),
            pltpu.VMEM((experts, width), bf),
            pltpu.VMEM((plane, top, rows), jnp.int32),
            pltpu.VMEM((2, width, ff), bf),
            pltpu.VMEM((2, width, ff), bf),
            pltpu.VMEM((2, ff, width), bf),
            pltpu.VMEM((pair, ff), bf),
            pltpu.VMEM((line, 2, pair, width), bf),
            pltpu.VMEM((experts, plane * rows), f32),
            pltpu.VMEM((plane, plane + 2, 2, rows), f32),
            pltpu.VMEM((2 * dp, 2, experts, cols), f32),
            pltpu.VMEM((2, ff, width), bf),
            pltpu.VMEM((2, rows, ff), bf),
            pltpu.VMEM((2, rows * KEPT // 8, ff), bf),
            dma((3,)), dma((2 * plane,)), dma((2 * plane,)),
            dma((1,)), dma((1,)), dma((1,)), dma((1,)), dma((3,)), dma((3,)), dma((1,)), dma((1,)),
            dma((1,)), dma((CHUNKS,)), dma((1,)), dma((CHUNKS,)), dma((1,)), dma((1,)),
            dma((4,)), dma((4,)), dma((1,)), dma((1,)), dma((7,)),
        ],
        compiler_params=pltpu.CompilerParams(
            collective_id=0, has_side_effects=True, vmem_limit_bytes=60 * 2**20),
    )(tokens, grad_out, router_weight.T, expert_index.T, w_gate, w_up, w_down)
    def finish(a, b, x, y):
        x[...] = a[...]
        y[...] = b[...]
    gg = pltpu.with_memory_space_constraint(gg, pltpu.VMEM)
    rg = pltpu.with_memory_space_constraint(rg, pltpu.VMEM)
    gg, rg = pl.pallas_call(
        finish,
        out_shape=(jax.ShapeDtypeStruct((top, rows), f32), jax.ShapeDtypeStruct((experts, cols), f32)),
        in_specs=[vmem, vmem],
        out_specs=(vmem, vmem),
    )(gg, rg)
    return gg.T, rg.T


def solution(mesh):
    n, dp = mesh.shape["expert"], mesh.shape["dp"]

    def on_device(tokens, grad_out, router_weight, expert_index, w_gate, w_up, w_down):
        rows, width = tokens.shape
        ff = w_gate.shape[2]
        held = 2 * (2 * n // 2 * rows * width * 2 + 8 * ff * width)
        fits = n % 4 == 0 and n // 4 == 4 and dp == 2 and held < 44 * 2**20 and width % (128 * n) == 0
        fits = fits and ff % (16 * dp * CHUNKS) == 0 and ff % 128 == 0
        fits = fits and rows % 128 == 0 and router_weight.shape[1] == n
        body = functools.partial(fused, n, dp) if fits else plain
        return body(tokens, grad_out, router_weight, expert_index, w_gate, w_up, w_down)

    in_specs = (
        P(("dp", "expert"), None),
        P(("dp", "expert"), None),
        P(),
        P(("dp", "expert"), None),
        P("expert", None, None),
        P("expert", None, None),
        P("expert", None, None),
    )
    out_specs = (P(("dp", "expert"), None), P("expert", None))
    return jax.shard_map(
        on_device, mesh=mesh, in_specs=in_specs, out_specs=out_specs, check_vma=False
    )
```

```python
import functools

import jax
import jax.numpy as jnp
from jax import lax
from jax.experimental import pallas as pl
from jax.experimental.pallas import tpu as pltpu
from jax.sharding import PartitionSpec as P


def plain(tokens, grad_out, router_weight, expert_index, w_gate, w_up, w_down):
    tok_rows, width = tokens.shape
    top = expert_index.shape[1]
    experts = router_weight.shape[1]
    me = lax.axis_index("expert")
    n = lax.axis_size("expert")
    index_all = lax.all_gather(expert_index, "expert", axis=0, tiled=True)
    tok_all = lax.all_gather(tokens, "expert", axis=0, tiled=True)
    grad_all = lax.all_gather(grad_out, "expert", axis=0, tiled=True)
    gate_in = jnp.dot(tok_all, w_gate[0], preferred_element_type=jnp.float32)
    up_in = jnp.dot(tok_all, w_up[0], preferred_element_type=jnp.float32)
    hidden = jax.nn.silu(gate_in) * up_in
    back = lax.dot_general(
        grad_all, w_down[0], (((1,), (1,)), ((), ())), preferred_element_type=jnp.float32
    )
    dots = jnp.sum(hidden * back, axis=1)
    dots_all = lax.all_gather(dots, "expert", axis=0).T
    labels = jnp.arange(experts, dtype=jnp.int32)
    picked = jnp.any(index_all[:, :, None] == labels, axis=1)
    logits = jnp.dot(tok_all, router_weight, preferred_element_type=jnp.float32)
    weights = jnp.where(picked, jnp.exp(jnp.where(picked, logits, 0.0)), 0.0)
    gates = weights / jnp.sum(weights, axis=1, keepdims=True)
    kept = jnp.where(picked, dots_all, 0.0)
    dense = gates * (kept - jnp.sum(gates * kept, axis=1, keepdims=True))
    cols = width // n
    mine = lax.dynamic_slice_in_dim(tok_all, me * cols, cols, axis=1)
    high = dense.astype(jnp.bfloat16)
    low = (dense - high.astype(jnp.float32)).astype(jnp.bfloat16)
    both = jnp.concatenate([high, low], axis=1)
    part = lax.dot_general(
        mine, both, (((0,), (0,)), ((), ())), preferred_element_type=jnp.float32
    )
    router_grad = lax.psum(part[:, :experts] + part[:, experts:], "dp")
    own = lax.dynamic_slice_in_dim(dots_all, me * tok_rows, tok_rows, axis=0)
    hits = (expert_index[:, :, None] == labels).astype(jnp.float32)
    gate_grad = jnp.sum(hits * own[:, None, :], axis=2)
    return (gate_grad, router_grad)


OUT, IN, SIDE = 0, 1, 2

END = {
    "start": [("S", "x", 3, 0, 0, IN, SIDE), ("S", "x", 3, 0, 1, IN, SIDE),
              ("S", "g", 3, 0, 0, IN), ("S", "g", 3, 0, 1, IN), ("send_down",)],
    "p0": [("F", "x", 2, 0, 0, SIDE), ("F", "x", 2, 0, 1, SIDE), ("W", "x", 3, 1, 0), ("W", "x", 3, 1, 1)],
    "p1": [("F", "x", 1, 0, 0, SIDE)],
    "p2": [("send_hidden", 0), ("F", "x", 1, 0, 1, SIDE), ("W", "x", 2, 1, 0), ("W", "x", 2, 1, 1)],
    "p3": [("F", "x", 0, 0, 0, SIDE)],
    "p4": [("send_hidden", 1), ("F", "x", 0, 0, 1, SIDE), ("W", "x", 1, 1, 0), ("W", "x", 1, 1, 1)],
    "p5": [("send_rest", 0), ("F", "g", 1, 0, 0, SIDE)],
    "r0": [],
    "r1": [("F", "g", 1, 0, 1, SIDE)],
    "p6": [("W", "x", 0, 1, 0), ("W", "x", 0, 1, 1)],
    "p7": [("F", "g", 0, 0, 0, SIDE)],
    "r2": [("F", "g", 0, 0, 1, SIDE)],
    "r3": [("W", "g", 1, 1, 0), ("W", "g", 1, 1, 1)],
    "r4": [("wait_rest", 1)],
    "r5": [("wait_rest", 0)],
    "r6": [("W", "g", 0, 1, 0), ("W", "g", 0, 1, 1)],
    "r7": [("W", "g", 2, 1, 0), ("W", "g", 2, 1, 1)],
    "last": [],
}
NEXT = {
    "start": [("S", "x", 2, 0, 0, OUT, IN, SIDE), ("S", "x", 2, 0, 1, OUT, IN, SIDE)],
    "p0": [("F", "x", 3, 0, 0, IN, SIDE), ("F", "x", 1, 0, 0, OUT, SIDE),
           ("F", "x", 3, 0, 1, IN, SIDE), ("F", "x", 1, 0, 1, OUT, SIDE),
           ("S", "g", 2, 0, 0, IN, SIDE), ("S", "g", 2, 0, 1, IN), ("W", "x", 2, 1, 0), ("W", "x", 2, 1, 1)],
    "p1": [("F", "g", 3, 0, 0, IN, SIDE), ("F", "x", 0, 0, 0, OUT, SIDE)],
    "p2": [("F", "x", 0, 0, 1, OUT), ("send_rest", 1), ("F", "g", 3, 0, 1, IN, SIDE), ("S", "g", 2, 0, 1, SIDE),
           ("W", "x", 3, 1, 0), ("F", "x", 3, 1, 1, IN), ("F", "g", 1, 0, 0, OUT), ("pass_down", 0)],
    "p3": [("pass_down", 1)],
    "p4": [("W", "x", 1, 1, 0), ("W", "x", 1, 1, 1), ("F", "g", 1, 0, 1, OUT, SIDE)],
    "p5": [("F", "g", 0, 0, 0, OUT), ("F", "g", 2, 1, 0, IN), ("pass_down", 2), ("cross_down", 0)],
    "r0": [("F", "g", 0, 0, 1, OUT), ("P", "g", 2, 1, 0, OUT), ("pass_down", 3), ("cross_down", 1)],
    "r1": [("F", "g", 3, 1, 0, IN)],
    "p6": [("pass_down", 4), ("W", "x", 0, 1, 1), ("W", "x", 0, 1, 0)],
    "p7": [("pass_down", 5), ("cross_down", 2)],
    "r2": [("F", "g", 3, 1, 1, IN), ("cross_down", 3), ("F", "g", 2, 1, 1, OUT)],
    "r3": [("cross_down", 4)],
    "r4": [],
    "r5": [],
    "r6": [("cross_down", 5), ("help", 0), ("W", "g", 0, 1, 0), ("W", "g", 0, 1, 1)],
    "r7": [("W", "g", 1, 1, 0), ("W", "g", 1, 1, 1)],
    "last": [("help", 1)],
}
BLOCKS = [((3, 0), (2, 0)), ((1, 0), (3, 0)), ((0, 0), (1, 0)), ((1, 1), (0, 0)),
          ((2, 0), (3, 1)), ((3, 1), (2, 1)), ((0, 1), (0, 1)), ((2, 1), (1, 1))]
EARLY = 2
CHUNKS = 6
KEPT = (6, 6)


def layer_kernel(n, dp, tok_in, grad_in, rw_in, idx_in, wg_in, wu_in, wd_in, gg_out, rg_out,
                 tok, grad, rw, idx, wg, wu, wd, hid, eo, lg, dots, part, far_wd, sent, more,
                 s_way, r_x, r_g, s_i, r_i, s_d, r_d, s_w, r_w, s_p, r_p,
                 s_f, r_f, s_fx, r_fx, s_fc, r_fc, s_h, r_h, s_t, r_t, loc):
    plane = n // 2
    line = plane // 2
    me = lax.axis_index("expert")
    xd = lax.axis_index("dp")
    c = me % 2
    q = me // 2
    y = q % 2
    z = q // 2
    rows, width = tok_in.shape
    ff = wg_in.shape[2]
    experts, top = rw_in.shape[0], idx_in.shape[0]
    pair = 2 * rows
    half = rows // 2
    upper = z // (line // 2)
    own = upper * z + (1 - upper) * (line - 1 - z)
    end = own - (line - 2)
    step = 2 * upper - 1

    def real(m):
        return upper * m + (1 - upper) * (line - 1 - m)

    def side(f):
        return y + f - 2 * y * f

    def dev(zz, yy, cc):
        return {"expert": (zz * 2 + yy) * 2 + cc}

    def remote(src, dst, ss, rs, where):
        return pltpu.make_async_remote_copy(
            src_ref=src, dst_ref=dst, send_sem=ss, recv_sem=rs,
            device_id=where, device_id_type=pl.DeviceIdType.MESH)

    def target(way):
        if way == OUT:
            return dev(z + step, y, c)
        if way == IN:
            return dev(z - step, y, c)
        return dev(z, 1 - y, c)

    kinds = {"x": (tok, r_x), "g": (grad, r_g)}

    def piece(kind, m, f, part_of, way):
        buf, rs = kinds[kind]
        zb, yb = real(m), side(f)
        at = buf.at[zb, pl.ds(pl.multiple_of(yb * rows + part_of * half, 16), half)]
        slot = (zb * 2 + yb) * 2 + part_of
        return remote(at, at, s_way.at[way], rs.at[slot], target(way))

    twin = {"dp": (xd + 1) % dp}
    mate = {"expert": q * 2 + (1 - c)}

    def down_rows(which, k):
        size = ff // dp // CHUNKS
        return pl.ds(pl.multiple_of(which * (ff // dp) + k * size, 16), size)

    def down(k):
        at = down_rows(xd, k)
        return remote(wd_in.at[0, at], far_wd.at[c, at], s_f.at[0], r_f.at[k], target(IN))

    def down_twin(k):
        at = far_wd.at[c, down_rows(xd, k)]
        return remote(at, at, s_fx.at[0], r_fx.at[k], twin)

    def down_mate(other, k):
        at = far_wd.at[c, down_rows((xd + other) % dp, k)]
        return remote(at, at, s_fc.at[0], r_fc.at[0], mate)

    fewer = (sent.shape[1], more.shape[1])
    rest = (rows - fewer[0], rows - fewer[1])

    def hidden_send(which, r):
        buf = more if which else sent
        return remote(buf.at[r], buf.at[r], s_h.at[2 * which + r], r_h.at[2 * which + r], target(IN))

    def rest_send(which, f, way):
        at = grad.at[real(line - 1 - which), pl.ds(pl.multiple_of(side(f) * rows + fewer[which], 16), rest[which])]
        return remote(at, at, s_t.at[which], r_t.at[which], target(way))

    def plane_dev(k):
        return {"expert": ((q + k) % plane) * 2 + c}

    def owner_dev(k):
        return {"dp": (xd + k // 2) % dp, "expert": q * 2 + (c + k) % 2}

    def few(buf, k, ss, rs):
        return remote(buf.at[pl.ds(0, k)], buf.at[pl.ds(0, k)], ss, rs, plane_dev(1))

    def block_dots(left, right):
        total = jnp.zeros((rows, 128), jnp.float32)
        for j in range(width // 128):
            total += left(j).astype(jnp.float32) * right(j).astype(jnp.float32)
        return jnp.sum(total.T, axis=0, keepdims=True)

    dt = width // 4 if width % 512 == 0 else width

    def help_end(which):
        if which == 0:
            remote(far_wd.at[0], far_wd.at[0], s_fc.at[0], r_fc.at[0], mate).wait_recv()
        buf = more if which else sent
        count = buf.shape[1]
        zb, base = (real(line - 2), y * rows) if which else (real(line - 1), (1 - y) * rows)
        theirs = pl.ds(pl.multiple_of(base, 16), count)

        @pl.loop(0, 2)
        def _(r):
            hidden_send(which, r).wait_recv()
            total = jnp.zeros((count, 128), jnp.float32)
            for j in range(width // dt):
                got = jnp.dot(buf[r], far_wd[r, :, j * dt:(j + 1) * dt],
                              preferred_element_type=jnp.float32).astype(jnp.bfloat16).astype(jnp.float32)
                for i in range(dt // 128):
                    lo = j * dt + i * 128
                    total += got[:, i * 128:(i + 1) * 128] * grad[
                        zb, theirs, lo:lo + 128].astype(jnp.float32)
            row = jnp.sum(total.T, axis=0, keepdims=True)
            if count < rows:
                row = jnp.concatenate([row, jnp.zeros((1, rows - count), jnp.float32)], axis=1)
            dots[q, plane + which, pl.ds(r, 1), :] = row

    def run(ops):
        for op in ops:
            if op[0] == "send_down":
                for k in range(CHUNKS):
                    down(k).start()
            elif op[0] == "send_hidden":
                hidden_send(op[1], 0).start()
                hidden_send(op[1], 1).start()
            elif op[0] == "send_rest":
                if rest[op[1]]:
                    rest_send(op[1], 0, OUT if op[1] else SIDE).start()
            elif op[0] == "wait_rest":
                if rest[op[1]]:
                    rest_send(op[1], 1 - op[1], SIDE).wait_recv()
            elif op[0] == "pass_down":
                down(op[1]).wait_recv()
                down_twin(op[1]).start()
                down_mate(0, op[1]).start()
            elif op[0] == "cross_down":
                down_twin(op[1]).wait_recv()
                down_mate(1, op[1]).start()
            elif op[0] == "help":
                help_end(op[1])
            else:
                what, kind, m, f, part_of = op[:5]
                if what in "FW":
                    piece(kind, m, f, part_of, SIDE).wait_recv()
                for way in op[5:]:
                    piece(kind, m, f, part_of, way).start()

    def slot(name):
        if END[name]:
            pl.when(end == 1)(lambda: run(END[name]))
        if NEXT[name]:
            pl.when(end == 0)(lambda: run(NEXT[name]))

    def sent_all(table):
        ways = [way for ops in table.values() for op in ops if op[0] in ("S", "F", "P") for way in op[5:]]
        for way in range(3):
            if way in ways:
                at = tok.at[:, pl.ds(0, ways.count(way) * half // line)]
                remote(at, at, s_way.at[way], r_x.at[0], target(SIDE)).wait_send()
        if table is END:
            at = far_wd.at[0, pl.ds(0, ff // dp)]
            remote(at, at, s_f.at[0], r_f.at[0], target(IN)).wait_send()
            for k in range(4):
                hidden_send(k // 2, k % 2).wait_send()
            if rest[0]:
                rest_send(0, 0, SIDE).wait_send()
            return
        at = far_wd.at[0, pl.ds(0, ff // dp)]
        remote(at, at, s_fx.at[0], r_fx.at[0], twin).wait_send()
        remote(far_wd.at[0], far_wd.at[0], s_fc.at[0], r_fc.at[0], mate).wait_send()
        if rest[1]:
            rest_send(1, 0, OUT).wait_send()

    barrier = pltpu.get_barrier_semaphore()

    def greet(where):
        pl.semaphore_signal(barrier, inc=1, device_id=where, device_id_type=pl.DeviceIdType.MESH)

    pl.when(end == 0)(lambda: greet(target(OUT)))
    greet(target(IN))
    greet(target(SIDE))
    for k in range(1, 2 * dp):
        greet(owner_dev(k))
    mine = pl.ds(pl.multiple_of(y * rows, 16), rows)
    local = [pltpu.make_async_copy(tok_in, tok.at[z, mine], loc.at[0]),
             pltpu.make_async_copy(grad_in, grad.at[z, mine], loc.at[1]),
             pltpu.make_async_copy(idx_in, idx.at[q], loc.at[2]),
             pltpu.make_async_copy(wg_in.at[0], wg.at[c], loc.at[3]),
             pltpu.make_async_copy(wu_in.at[0], wu.at[c], loc.at[4]),
             pltpu.make_async_copy(wd_in.at[0], wd.at[c], loc.at[5]),
             pltpu.make_async_copy(rw_in, rw, loc.at[6])]
    for copy in local[:2]:
        copy.start()
    pl.when(end == 0)(lambda: pl.semaphore_wait(barrier, 2 + 2 * dp))
    pl.when(end == 1)(lambda: pl.semaphore_wait(barrier, 1 + 2 * dp))

    for copy in local[:2]:
        copy.wait()
    slot("start")
    for copy in local[2:]:
        copy.start()
    weights = [remote(wg_in.at[0], wg.at[c], s_w.at[0], r_w.at[0], mate),
               remote(wu_in.at[0], wu.at[c], s_w.at[1], r_w.at[1], mate),
               remote(wd_in.at[0], wd.at[c], s_w.at[2], r_w.at[2], mate)]
    for w in weights:
        w.start()
    index_sends = [remote(idx_in, idx.at[q], s_i.at[0], r_i.at[0], plane_dev(k)) for k in range(1, plane)]

    ft = ff // 3 if ff % 384 == 0 else ff

    def produce(zp, r, first, keep):
        @pl.loop(0, ff // ft)
        def _(j):
            at = pl.ds(pl.multiple_of(j * ft, 128), ft)
            x = tok[zp]
            g = jnp.dot(x, wg[r, :, at], preferred_element_type=jnp.float32)
            u = jnp.dot(x, wu[r, :, at], preferred_element_type=jnp.float32)
            hid[:, at] = (g / (1.0 + jnp.exp(-g)) * u).astype(jnp.bfloat16)

        if keep == 0:
            @pl.when(end == 1)
            def _():
                sent[r] = hid[pl.ds(pl.multiple_of((1 - y) * rows, 16), fewer[0]), :]
        if keep == 1:
            @pl.when(end == 1)
            def _():
                more[r] = hid[pl.ds(pl.multiple_of(y * rows, 16), fewer[1]), :]

        @pl.loop(0, width // dt)
        def _(j):
            at = pl.ds(pl.multiple_of(j * dt, 128), dt)
            eo[zp, r, :, at] = jnp.dot(
                hid[...], wd[r, :, at], preferred_element_type=jnp.float32).astype(jnp.bfloat16)
        if first:
            lg[:, pl.ds(pl.multiple_of(zp * pair, 128), pair)] = lax.dot_general(
                rw[...], tok[zp], (((1,), (1,)), ((), ())), preferred_element_type=jnp.float32)

    def reduce_block(zb, yb):
        at = pl.ds(pl.multiple_of(yb * rows, 16), rows)

        @pl.loop(0, 2)
        def _(r):
            row = block_dots(lambda j: eo[zb, r, at, j * 128:(j + 1) * 128],
                             lambda j: grad[zb, at, j * 128:(j + 1) * 128])
            dots[q, zb * 2 + yb, pl.ds(r, 1), :] = row

    def reduce_some(lo, hi):
        for i in range(lo, hi):
            slot("r" + str(i))
            a, b = BLOCKS[i]
            m = end * a[0] + (1 - end) * b[0]
            f = end * a[1] + (1 - end) * b[1]
            if (rest[0] or a != (3, 1)) and (rest[1] or a != (2, 0)):
                reduce_block(real(m), side(f))
            else:
                pl.when(end == 0)(lambda: reduce_block(real(m), side(f)))

    order = [2 + end, 3 - end, 1, 0]
    for i in range(line):
        if i == line - 1:
            reduce_some(0, EARLY)
        for k in range(2):
            slot("p" + str(2 * i + k))
            if i == 0 and k == 0:
                for copy in local[2:]:
                    copy.wait()
            if i == 0 and k == 1:
                for w in weights:
                    w.wait_recv()
            produce(real(order[i]), c + k - 2 * c * k, k == 0, i)

    for w in index_sends:
        w.start()

    reduce_some(EARLY, len(BLOCKS))
    slot("last")

    dot_sends = [remote(dots.at[q], dots.at[q], s_d.at[0], r_d.at[0], plane_dev(k)) for k in range(1, plane)]
    for w in dot_sends:
        w.start()
    few(idx, plane - 1, s_i.at[0], r_i.at[0]).wait()
    labels = lax.broadcasted_iota(jnp.int32, (experts, plane * rows), 0)
    chosen = jnp.zeros((experts, plane * rows), jnp.float32)
    for k in range(top):
        named = jnp.concatenate([idx[b, pl.ds(k, 1), :] for b in range(plane)], axis=1)
        chosen = jnp.where(labels == named, 1.0, chosen)
    weight = jnp.where(chosen > 0.0, jnp.exp(jnp.where(chosen > 0.0, lg[...], 0.0)), 0.0)
    gates = weight / jnp.sum(weight, axis=0, keepdims=True)
    ends = (0, 1, plane - 2, plane - 1)
    few(dots, plane - 1, s_d.at[0], r_d.at[0]).wait()
    lanes = lax.broadcasted_iota(jnp.int32, (2, rows), 1)

    def next_to(b):
        return b + 2 if b < 2 else b - 2

    def patched(b, which):
        helped = dots[next_to(b), plane + which]
        mine_at = next_to(b) if which else b ^ 1
        return jnp.where(lanes < fewer[which], helped, dots[b, mine_at]) if rest[which] else helped

    def dots_of(b):
        blocks = [dots[b, k] for k in range(plane)]
        if b in ends:
            blocks[b ^ 1] = patched(b, 0)
            blocks[next_to(b)] = patched(b, 1)
        return jnp.concatenate(blocks, axis=1)

    all_dots = jnp.concatenate([dots_of(b) for b in range(plane)], axis=0)
    kept = jnp.where(chosen > 0.0, all_dots, 0.0)
    dense = gates * (kept - jnp.sum(gates * kept, axis=0, keepdims=True))
    high = dense.astype(jnp.bfloat16)
    low = (dense - high.astype(jnp.float32)).astype(jnp.bfloat16)
    cols = width // n
    at = pl.ds(pl.multiple_of(q * 2 * cols, 128), 2 * cols)
    both = jnp.concatenate([high, low], axis=0)
    split = jnp.zeros((2 * experts, 2 * cols), jnp.float32)
    for b in range(line):
        split += jnp.dot(both[:, b * pair:(b + 1) * pair], tok[b, :, at], preferred_element_type=jnp.float32)
    terms = split[:experts] + split[experts:]
    part[0, 0] = terms[:, :cols]
    part[0, 1] = terms[:, cols:]
    part_sends = [remote(part.at[0, (c + k) % 2], part.at[k, 0], s_p.at[0], r_p.at[0], owner_dev(k))
                  for k in range(1, 2 * dp)]
    for w in part_sends:
        w.start()
    held = []
    for b in range(plane):
        row = dots[b, q]
        if b in ends:
            row = jnp.where(q == (b ^ 1), patched(b, 0), jnp.where(q == next_to(b), patched(b, 1), row))
        held.append(row)
    held = jnp.concatenate(held, axis=0)
    names = idx[q]
    small = lax.broadcasted_iota(jnp.int32, (experts, rows), 0)
    for k in range(top):
        gg_out[pl.ds(k, 1), :] = jnp.sum(
            jnp.where(small == names[k:k + 1, :], held, 0.0), axis=0, keepdims=True)
    for w in weights:
        w.wait_send()
    pl.when(end == 1)(lambda: sent_all(END))
    pl.when(end == 0)(lambda: sent_all(NEXT))
    at = part.at[pl.ds(0, 2 * dp - 1), 0]
    remote(at, at, s_p.at[0], r_p.at[0], mate).wait()
    total = part[0, c]
    for k in range(1, 2 * dp):
        total += part[k, 0]
    rg_out[...] = total


def fused(n, dp, tokens, grad_out, router_weight, expert_index, w_gate, w_up, w_down):
    rows, width = tokens.shape
    ff = w_gate.shape[2]
    top = expert_index.shape[1]
    experts = router_weight.shape[1]
    plane, cols = n // 2, width // n
    line = plane // 2
    pair = 2 * rows
    anywhere = pl.BlockSpec(memory_space=pl.ANY)
    vmem = pl.BlockSpec(memory_space=pltpu.VMEM)
    dma = pltpu.SemaphoreType.DMA
    bf, f32 = jnp.bfloat16, jnp.float32
    gg, rg = pl.pallas_call(
        functools.partial(layer_kernel, n, dp),
        out_shape=(pltpu.VMEM((top, rows), f32), pltpu.VMEM((experts, cols), f32)),
        in_specs=[anywhere] * 7,
        out_specs=(vmem, vmem),
        scratch_shapes=[
            pltpu.VMEM((line, pair, width), bf),
            pltpu.VMEM((line, pair, width), bf),
            pltpu.VMEM((experts, width), bf),
            pltpu.VMEM((plane, top, rows), jnp.int32),
            pltpu.VMEM((2, width, ff), bf),
            pltpu.VMEM((2, width, ff), bf),
            pltpu.VMEM((2, ff, width), bf),
            pltpu.VMEM((pair, ff), bf),
            pltpu.VMEM((line, 2, pair, width), bf),
            pltpu.VMEM((experts, plane * rows), f32),
            pltpu.VMEM((plane, plane + 2, 2, rows), f32),
            pltpu.VMEM((2 * dp, 2, experts, cols), f32),
            pltpu.VMEM((2, ff, width), bf),
            pltpu.VMEM((2, rows * KEPT[0] // 8, ff), bf),
            pltpu.VMEM((2, rows * KEPT[1] // 8, ff), bf),
            dma((3,)), dma((2 * plane,)), dma((2 * plane,)),
            dma((1,)), dma((1,)), dma((1,)), dma((1,)), dma((3,)), dma((3,)), dma((1,)), dma((1,)),
            dma((1,)), dma((CHUNKS,)), dma((1,)), dma((CHUNKS,)), dma((1,)), dma((1,)),
            dma((4,)), dma((4,)), dma((2,)), dma((2,)), dma((7,)),
        ],
        compiler_params=pltpu.CompilerParams(
            collective_id=0, has_side_effects=True, vmem_limit_bytes=60 * 2**20),
    )(tokens, grad_out, router_weight.T, expert_index.T, w_gate, w_up, w_down)
    def finish(a, b, x, y):
        x[...] = a[...]
        y[...] = b[...]
    gg = pltpu.with_memory_space_constraint(gg, pltpu.VMEM)
    rg = pltpu.with_memory_space_constraint(rg, pltpu.VMEM)
    gg, rg = pl.pallas_call(
        finish,
        out_shape=(jax.ShapeDtypeStruct((top, rows), f32), jax.ShapeDtypeStruct((experts, cols), f32)),
        in_specs=[vmem, vmem],
        out_specs=(vmem, vmem),
    )(gg, rg)
    return gg.T, rg.T


def solution(mesh):
    n, dp = mesh.shape["expert"], mesh.shape["dp"]

    def on_device(tokens, grad_out, router_weight, expert_index, w_gate, w_up, w_down):
        rows, width = tokens.shape
        ff = w_gate.shape[2]
        held = 2 * (2 * n // 2 * rows * width * 2 + 8 * ff * width)
        fits = n % 4 == 0 and n // 4 == 4 and dp == 2 and held < 44 * 2**20 and width % (128 * n) == 0
        fits = fits and ff % (16 * dp * CHUNKS) == 0 and ff % 128 == 0
        fits = fits and rows % 128 == 0 and router_weight.shape[1] == n
        body = functools.partial(fused, n, dp) if fits else plain
        return body(tokens, grad_out, router_weight, expert_index, w_gate, w_up, w_down)

    in_specs = (
        P(("dp", "expert"), None),
        P(("dp", "expert"), None),
        P(),
        P(("dp", "expert"), None),
        P("expert", None, None),
        P("expert", None, None),
        P("expert", None, None),
    )
    out_specs = (P(("dp", "expert"), None), P("expert", None))
    return jax.shard_map(
        on_device, mesh=mesh, in_specs=in_specs, out_specs=out_specs, check_vma=False
    )
```

```python
import functools

import jax
import jax.numpy as jnp
from jax import lax
from jax.experimental import pallas as pl
from jax.experimental.pallas import tpu as pltpu
from jax.sharding import PartitionSpec as P


def plain(tokens, grad_out, router_weight, expert_index, w_gate, w_up, w_down):
    tok_rows, width = tokens.shape
    top = expert_index.shape[1]
    experts = router_weight.shape[1]
    me = lax.axis_index("expert")
    n = lax.axis_size("expert")
    index_all = lax.all_gather(expert_index, "expert", axis=0, tiled=True)
    tok_all = lax.all_gather(tokens, "expert", axis=0, tiled=True)
    grad_all = lax.all_gather(grad_out, "expert", axis=0, tiled=True)
    gate_in = jnp.dot(tok_all, w_gate[0], preferred_element_type=jnp.float32)
    up_in = jnp.dot(tok_all, w_up[0], preferred_element_type=jnp.float32)
    hidden = jax.nn.silu(gate_in) * up_in
    back = lax.dot_general(
        grad_all, w_down[0], (((1,), (1,)), ((), ())), preferred_element_type=jnp.float32
    )
    dots = jnp.sum(hidden * back, axis=1)
    dots_all = lax.all_gather(dots, "expert", axis=0).T
    labels = jnp.arange(experts, dtype=jnp.int32)
    picked = jnp.any(index_all[:, :, None] == labels, axis=1)
    logits = jnp.dot(tok_all, router_weight, preferred_element_type=jnp.float32)
    weights = jnp.where(picked, jnp.exp(jnp.where(picked, logits, 0.0)), 0.0)
    gates = weights / jnp.sum(weights, axis=1, keepdims=True)
    kept = jnp.where(picked, dots_all, 0.0)
    dense = gates * (kept - jnp.sum(gates * kept, axis=1, keepdims=True))
    cols = width // n
    mine = lax.dynamic_slice_in_dim(tok_all, me * cols, cols, axis=1)
    high = dense.astype(jnp.bfloat16)
    low = (dense - high.astype(jnp.float32)).astype(jnp.bfloat16)
    both = jnp.concatenate([high, low], axis=1)
    part = lax.dot_general(
        mine, both, (((0,), (0,)), ((), ())), preferred_element_type=jnp.float32
    )
    router_grad = lax.psum(part[:, :experts] + part[:, experts:], "dp")
    own = lax.dynamic_slice_in_dim(dots_all, me * tok_rows, tok_rows, axis=0)
    hits = (expert_index[:, :, None] == labels).astype(jnp.float32)
    gate_grad = jnp.sum(hits * own[:, None, :], axis=2)
    return (gate_grad, router_grad)


OUT, IN, SIDE = 0, 1, 2

END = {
    "start": [("S", "x", 3, 0, 0, IN, SIDE), ("S", "x", 3, 0, 1, IN, SIDE),
              ("S", "g", 3, 0, 0, IN), ("S", "g", 3, 0, 1, IN), ("send_down",)],
    "p0": [("F", "x", 2, 0, 0, SIDE), ("F", "x", 2, 0, 1, SIDE), ("W", "x", 3, 1, 0), ("W", "x", 3, 1, 1)],
    "p1": [("F", "x", 1, 0, 0, SIDE)],
    "p2": [("send_hidden", 0), ("F", "x", 1, 0, 1, SIDE), ("W", "x", 2, 1, 0), ("W", "x", 2, 1, 1)],
    "p3": [("F", "x", 0, 0, 0, SIDE)],
    "p4": [("send_hidden", 1), ("F", "x", 0, 0, 1, SIDE), ("W", "x", 1, 1, 0), ("W", "x", 1, 1, 1)],
    "p5": [("send_rest", 0), ("F", "g", 1, 0, 0, SIDE)],
    "r0": [],
    "r1": [("F", "g", 1, 0, 1, SIDE)],
    "p6": [("W", "x", 0, 1, 0), ("W", "x", 0, 1, 1)],
    "p7": [("F", "g", 0, 0, 0, SIDE)],
    "r2": [("F", "g", 0, 0, 1, SIDE)],
    "r3": [("W", "g", 1, 1, 0), ("W", "g", 1, 1, 1)],
    "r4": [("wait_rest", 1)],
    "r5": [("wait_rest", 0)],
    "r6": [("W", "g", 0, 1, 0), ("W", "g", 0, 1, 1)],
    "r7": [("W", "g", 2, 1, 0), ("W", "g", 2, 1, 1)],
    "last": [],
}
NEXT = {
    "start": [("S", "x", 2, 0, 0, OUT, IN, SIDE), ("S", "x", 2, 0, 1, OUT, IN, SIDE)],
    "p0": [("F", "x", 3, 0, 0, IN, SIDE), ("F", "x", 1, 0, 0, OUT, SIDE),
           ("F", "x", 3, 0, 1, IN, SIDE), ("F", "x", 1, 0, 1, OUT, SIDE),
           ("S", "g", 2, 0, 0, IN, SIDE), ("S", "g", 2, 0, 1, IN), ("W", "x", 2, 1, 0), ("W", "x", 2, 1, 1)],
    "p1": [("F", "g", 3, 0, 0, IN, SIDE), ("F", "x", 0, 0, 0, OUT, SIDE)],
    "p2": [("F", "x", 0, 0, 1, OUT), ("send_rest", 1), ("F", "g", 3, 0, 1, IN, SIDE), ("S", "g", 2, 0, 1, SIDE),
           ("W", "x", 3, 1, 0), ("F", "x", 3, 1, 1, IN), ("F", "g", 1, 0, 0, OUT), ("pass_down", 0)],
    "p3": [("pass_down", 1)],
    "p4": [("W", "x", 1, 1, 0), ("W", "x", 1, 1, 1), ("F", "g", 1, 0, 1, OUT, SIDE)],
    "p5": [("F", "g", 0, 0, 0, OUT), ("F", "g", 2, 1, 0, IN), ("pass_down", 2), ("cross_down", 0)],
    "r0": [("F", "g", 0, 0, 1, OUT), ("P", "g", 2, 1, 0, OUT), ("pass_down", 3), ("cross_down", 1)],
    "r1": [("F", "g", 3, 1, 0, IN)],
    "p6": [("pass_down", 4), ("W", "x", 0, 1, 1), ("W", "x", 0, 1, 0)],
    "p7": [("pass_down", 5), ("cross_down", 2)],
    "r2": [("F", "g", 3, 1, 1, IN), ("cross_down", 3), ("F", "g", 2, 1, 1, OUT)],
    "r3": [("cross_down", 4)],
    "r4": [],
    "r5": [],
    "r6": [("cross_down", 5), ("help", 0), ("W", "g", 0, 1, 0), ("W", "g", 0, 1, 1)],
    "r7": [("W", "g", 1, 1, 0), ("W", "g", 1, 1, 1)],
    "last": [("help", 1)],
}
BLOCKS = [((3, 0), (2, 0)), ((1, 0), (3, 0)), ((0, 0), (1, 0)), ((1, 1), (0, 0)),
          ((2, 0), (3, 1)), ((3, 1), (2, 1)), ((0, 1), (0, 1)), ((2, 1), (1, 1))]
EARLY = 2
CHUNKS = 6
KEPT = (7, 6)


def layer_kernel(n, dp, tok_in, grad_in, rw_in, idx_in, wg_in, wu_in, wd_in, gg_out, rg_out,
                 tok, grad, rw, idx, wg, wu, wd, hid, eo, lg, dots, part, far_wd, sent, more,
                 s_way, r_x, r_g, s_i, r_i, s_d, r_d, s_w, r_w, s_p, r_p,
                 s_f, r_f, s_fx, r_fx, s_fc, r_fc, s_h, r_h, s_t, r_t, loc):
    plane = n // 2
    line = plane // 2
    me = lax.axis_index("expert")
    xd = lax.axis_index("dp")
    c = me % 2
    q = me // 2
    y = q % 2
    z = q // 2
    rows, width = tok_in.shape
    ff = wg_in.shape[2]
    experts, top = rw_in.shape[0], idx_in.shape[0]
    pair = 2 * rows
    half = rows // 2
    upper = z // (line // 2)
    own = upper * z + (1 - upper) * (line - 1 - z)
    end = own - (line - 2)
    step = 2 * upper - 1

    def real(m):
        return upper * m + (1 - upper) * (line - 1 - m)

    def side(f):
        return y + f - 2 * y * f

    def dev(zz, yy, cc):
        return {"expert": (zz * 2 + yy) * 2 + cc}

    def remote(src, dst, ss, rs, where):
        return pltpu.make_async_remote_copy(
            src_ref=src, dst_ref=dst, send_sem=ss, recv_sem=rs,
            device_id=where, device_id_type=pl.DeviceIdType.MESH)

    def target(way):
        if way == OUT:
            return dev(z + step, y, c)
        if way == IN:
            return dev(z - step, y, c)
        return dev(z, 1 - y, c)

    kinds = {"x": (tok, r_x), "g": (grad, r_g)}

    def piece(kind, m, f, part_of, way):
        buf, rs = kinds[kind]
        zb, yb = real(m), side(f)
        at = buf.at[zb, pl.ds(pl.multiple_of(yb * rows + part_of * half, 16), half)]
        slot = (zb * 2 + yb) * 2 + part_of
        return remote(at, at, s_way.at[way], rs.at[slot], target(way))

    twin = {"dp": (xd + 1) % dp}
    mate = {"expert": q * 2 + (1 - c)}

    def down_rows(which, k):
        size = ff // dp // CHUNKS
        return pl.ds(pl.multiple_of(which * (ff // dp) + k * size, 16), size)

    def down(k):
        at = down_rows(xd, k)
        return remote(wd_in.at[0, at], far_wd.at[c, at], s_f.at[0], r_f.at[k], target(IN))

    def down_twin(k):
        at = far_wd.at[c, down_rows(xd, k)]
        return remote(at, at, s_fx.at[0], r_fx.at[k], twin)

    def down_mate(other, k):
        at = far_wd.at[c, down_rows((xd + other) % dp, k)]
        return remote(at, at, s_fc.at[0], r_fc.at[0], mate)

    fewer = (sent.shape[1], more.shape[1])
    rest = (rows - fewer[0], rows - fewer[1])

    def hidden_send(which, r):
        buf = more if which else sent
        return remote(buf.at[r], buf.at[r], s_h.at[2 * which + r], r_h.at[2 * which + r], target(IN))

    def rest_send(which, f, way):
        at = grad.at[real(line - 1 - which), pl.ds(pl.multiple_of(side(f) * rows + fewer[which], 16), rest[which])]
        return remote(at, at, s_t.at[which], r_t.at[which], target(way))

    def plane_dev(k):
        return {"expert": ((q + k) % plane) * 2 + c}

    def owner_dev(k):
        return {"dp": (xd + k // 2) % dp, "expert": q * 2 + (c + k) % 2}

    def few(buf, k, ss, rs):
        return remote(buf.at[pl.ds(0, k)], buf.at[pl.ds(0, k)], ss, rs, plane_dev(1))

    def block_dots(left, right):
        total = jnp.zeros((rows, 128), jnp.float32)
        for j in range(width // 128):
            total += left(j).astype(jnp.float32) * right(j).astype(jnp.float32)
        return jnp.sum(total.T, axis=0, keepdims=True)

    dt = width // 4 if width % 512 == 0 else width

    def help_end(which):
        if which == 0:
            remote(far_wd.at[0], far_wd.at[0], s_fc.at[0], r_fc.at[0], mate).wait_recv()
        buf = more if which else sent
        count = buf.shape[1]
        zb, base = (real(line - 2), y * rows) if which else (real(line - 1), (1 - y) * rows)
        theirs = pl.ds(pl.multiple_of(base, 16), count)

        @pl.loop(0, 2)
        def _(r):
            hidden_send(which, r).wait_recv()
            total = jnp.zeros((count, 128), jnp.float32)
            for j in range(width // dt):
                got = jnp.dot(buf[r], far_wd[r, :, j * dt:(j + 1) * dt],
                              preferred_element_type=jnp.float32).astype(jnp.bfloat16).astype(jnp.float32)
                for i in range(dt // 128):
                    lo = j * dt + i * 128
                    total += got[:, i * 128:(i + 1) * 128] * grad[
                        zb, theirs, lo:lo + 128].astype(jnp.float32)
            row = jnp.sum(total.T, axis=0, keepdims=True)
            if count < rows:
                row = jnp.concatenate([row, jnp.zeros((1, rows - count), jnp.float32)], axis=1)
            dots[q, plane + which, pl.ds(r, 1), :] = row

    def run(ops):
        for op in ops:
            if op[0] == "send_down":
                for k in range(CHUNKS):
                    down(k).start()
            elif op[0] == "send_hidden":
                hidden_send(op[1], 0).start()
                hidden_send(op[1], 1).start()
            elif op[0] == "send_rest":
                if rest[op[1]]:
                    rest_send(op[1], 0, OUT if op[1] else SIDE).start()
            elif op[0] == "wait_rest":
                if rest[op[1]]:
                    rest_send(op[1], 1 - op[1], SIDE).wait_recv()
            elif op[0] == "pass_down":
                down(op[1]).wait_recv()
                down_twin(op[1]).start()
                down_mate(0, op[1]).start()
            elif op[0] == "cross_down":
                down_twin(op[1]).wait_recv()
                down_mate(1, op[1]).start()
            elif op[0] == "help":
                help_end(op[1])
            else:
                what, kind, m, f, part_of = op[:5]
                if what in "FW":
                    piece(kind, m, f, part_of, SIDE).wait_recv()
                for way in op[5:]:
                    piece(kind, m, f, part_of, way).start()

    def slot(name):
        if END[name]:
            pl.when(end == 1)(lambda: run(END[name]))
        if NEXT[name]:
            pl.when(end == 0)(lambda: run(NEXT[name]))

    def sent_all(table):
        ways = [way for ops in table.values() for op in ops if op[0] in ("S", "F", "P") for way in op[5:]]
        for way in range(3):
            if way in ways:
                at = tok.at[:, pl.ds(0, ways.count(way) * half // line)]
                remote(at, at, s_way.at[way], r_x.at[0], target(SIDE)).wait_send()
        if table is END:
            at = far_wd.at[0, pl.ds(0, ff // dp)]
            remote(at, at, s_f.at[0], r_f.at[0], target(IN)).wait_send()
            for k in range(4):
                hidden_send(k // 2, k % 2).wait_send()
            if rest[0]:
                rest_send(0, 0, SIDE).wait_send()
            return
        at = far_wd.at[0, pl.ds(0, ff // dp)]
        remote(at, at, s_fx.at[0], r_fx.at[0], twin).wait_send()
        remote(far_wd.at[0], far_wd.at[0], s_fc.at[0], r_fc.at[0], mate).wait_send()
        if rest[1]:
            rest_send(1, 0, OUT).wait_send()

    barrier = pltpu.get_barrier_semaphore()

    def greet(where):
        pl.semaphore_signal(barrier, inc=1, device_id=where, device_id_type=pl.DeviceIdType.MESH)

    pl.when(end == 0)(lambda: greet(target(OUT)))
    greet(target(IN))
    greet(target(SIDE))
    for k in range(1, 2 * dp):
        greet(owner_dev(k))
    mine = pl.ds(pl.multiple_of(y * rows, 16), rows)
    local = [pltpu.make_async_copy(tok_in, tok.at[z, mine], loc.at[0]),
             pltpu.make_async_copy(grad_in, grad.at[z, mine], loc.at[1]),
             pltpu.make_async_copy(idx_in, idx.at[q], loc.at[2]),
             pltpu.make_async_copy(wg_in.at[0], wg.at[c], loc.at[3]),
             pltpu.make_async_copy(wu_in.at[0], wu.at[c], loc.at[4]),
             pltpu.make_async_copy(wd_in.at[0], wd.at[c], loc.at[5]),
             pltpu.make_async_copy(rw_in, rw, loc.at[6])]
    for copy in local[:2]:
        copy.start()
    pl.when(end == 0)(lambda: pl.semaphore_wait(barrier, 2 + 2 * dp))
    pl.when(end == 1)(lambda: pl.semaphore_wait(barrier, 1 + 2 * dp))

    for copy in local[:2]:
        copy.wait()
    slot("start")
    for copy in local[2:]:
        copy.start()
    weights = [remote(wg_in.at[0], wg.at[c], s_w.at[0], r_w.at[0], mate),
               remote(wu_in.at[0], wu.at[c], s_w.at[1], r_w.at[1], mate),
               remote(wd_in.at[0], wd.at[c], s_w.at[2], r_w.at[2], mate)]
    for w in weights:
        w.start()
    index_sends = [remote(idx_in, idx.at[q], s_i.at[0], r_i.at[0], plane_dev(k)) for k in range(1, plane)]

    ft = ff // 3 if ff % 384 == 0 else ff

    def produce(zp, r, first, keep):
        @pl.loop(0, ff // ft)
        def _(j):
            at = pl.ds(pl.multiple_of(j * ft, 128), ft)
            x = tok[zp]
            g = jnp.dot(x, wg[r, :, at], preferred_element_type=jnp.float32)
            u = jnp.dot(x, wu[r, :, at], preferred_element_type=jnp.float32)
            hid[:, at] = (g / (1.0 + jnp.exp(-g)) * u).astype(jnp.bfloat16)

        if keep == 0:
            @pl.when(end == 1)
            def _():
                sent[r] = hid[pl.ds(pl.multiple_of((1 - y) * rows, 16), fewer[0]), :]
        if keep == 1:
            @pl.when(end == 1)
            def _():
                more[r] = hid[pl.ds(pl.multiple_of(y * rows, 16), fewer[1]), :]

        @pl.loop(0, width // dt)
        def _(j):
            at = pl.ds(pl.multiple_of(j * dt, 128), dt)
            eo[zp, r, :, at] = jnp.dot(
                hid[...], wd[r, :, at], preferred_element_type=jnp.float32).astype(jnp.bfloat16)
        if first:
            lg[:, pl.ds(pl.multiple_of(zp * pair, 128), pair)] = lax.dot_general(
                rw[...], tok[zp], (((1,), (1,)), ((), ())), preferred_element_type=jnp.float32)

    def reduce_block(zb, yb):
        at = pl.ds(pl.multiple_of(yb * rows, 16), rows)

        @pl.loop(0, 2)
        def _(r):
            row = block_dots(lambda j: eo[zb, r, at, j * 128:(j + 1) * 128],
                             lambda j: grad[zb, at, j * 128:(j + 1) * 128])
            dots[q, zb * 2 + yb, pl.ds(r, 1), :] = row

    def reduce_some(lo, hi):
        for i in range(lo, hi):
            slot("r" + str(i))
            a, b = BLOCKS[i]
            m = end * a[0] + (1 - end) * b[0]
            f = end * a[1] + (1 - end) * b[1]
            if (rest[0] or a != (3, 1)) and (rest[1] or a != (2, 0)):
                reduce_block(real(m), side(f))
            else:
                pl.when(end == 0)(lambda: reduce_block(real(m), side(f)))

    order = [2 + end, 3 - end, 1, 0]
    for i in range(line):
        if i == line - 1:
            reduce_some(0, EARLY)
        for k in range(2):
            slot("p" + str(2 * i + k))
            if i == 0 and k == 0:
                for copy in local[2:]:
                    copy.wait()
            if i == 0 and k == 1:
                for w in weights:
                    w.wait_recv()
            produce(real(order[i]), c + k - 2 * c * k, k == 0, i)

    for w in index_sends:
        w.start()

    reduce_some(EARLY, len(BLOCKS))
    slot("last")

    def dot_sends(blocks, which):
        at = dots.at[q, pl.ds(0, blocks)]
        for k in range(1, plane):
            remote(at, at, s_d.at[0], r_d.at[which], plane_dev(k)).start()

    pl.when(end == 1)(lambda: dot_sends(plane, 0))
    pl.when(end == 0)(lambda: dot_sends(plane + 2, 1))
    few(idx, plane - 1, s_i.at[0], r_i.at[0]).wait()
    labels = lax.broadcasted_iota(jnp.int32, (experts, plane * rows), 0)
    chosen = jnp.zeros((experts, plane * rows), jnp.float32)
    for k in range(top):
        named = jnp.concatenate([idx[b, pl.ds(k, 1), :] for b in range(plane)], axis=1)
        chosen = jnp.where(labels == named, 1.0, chosen)
    weight = jnp.where(chosen > 0.0, jnp.exp(jnp.where(chosen > 0.0, lg[...], 0.0)), 0.0)
    gates = weight / jnp.sum(weight, axis=0, keepdims=True)
    ends = (0, 1, plane - 2, plane - 1)

    def dots_wait(own_blocks, from_ends, from_next):
        at = dots.at[pl.ds(0, plane - 1), pl.ds(0, own_blocks)]
        remote(at, at, s_d.at[0], r_d.at[0], mate).wait_send()
        at = dots.at[pl.ds(0, from_ends), pl.ds(0, plane)]
        remote(at, at, s_d.at[0], r_d.at[0], mate).wait_recv()
        at = dots.at[pl.ds(0, from_next), pl.ds(0, plane + 2)]
        remote(at, at, s_d.at[0], r_d.at[1], mate).wait_recv()

    pl.when(end == 1)(lambda: dots_wait(plane, 3, 4))
    pl.when(end == 0)(lambda: dots_wait(plane + 2, 4, 3))
    lanes = lax.broadcasted_iota(jnp.int32, (2, rows), 1)

    def next_to(b):
        return b + 2 if b < 2 else b - 2

    def patched(b, which):
        helped = dots[next_to(b), plane + which]
        mine_at = next_to(b) if which else b ^ 1
        return jnp.where(lanes < fewer[which], helped, dots[b, mine_at]) if rest[which] else helped

    def dots_of(b):
        blocks = [dots[b, k] for k in range(plane)]
        if b in ends:
            blocks[b ^ 1] = patched(b, 0)
            blocks[next_to(b)] = patched(b, 1)
        return jnp.concatenate(blocks, axis=1)

    all_dots = jnp.concatenate([dots_of(b) for b in range(plane)], axis=0)
    kept = jnp.where(chosen > 0.0, all_dots, 0.0)
    dense = gates * (kept - jnp.sum(gates * kept, axis=0, keepdims=True))
    high = dense.astype(jnp.bfloat16)
    low = (dense - high.astype(jnp.float32)).astype(jnp.bfloat16)
    cols = width // n
    at = pl.ds(pl.multiple_of(q * 2 * cols, 128), 2 * cols)
    both = jnp.concatenate([high, low], axis=0)
    split = jnp.zeros((2 * experts, 2 * cols), jnp.float32)
    for b in range(line):
        split += jnp.dot(both[:, b * pair:(b + 1) * pair], tok[b, :, at], preferred_element_type=jnp.float32)
    terms = split[:experts] + split[experts:]
    part[0, 0] = terms[:, :cols]
    part[0, 1] = terms[:, cols:]
    part_sends = [remote(part.at[0, (c + k) % 2], part.at[k, 0], s_p.at[0], r_p.at[0], owner_dev(k))
                  for k in range(1, 2 * dp)]
    for w in part_sends:
        w.start()
    held = []
    for b in range(plane):
        row = dots[b, q]
        if b in ends:
            row = jnp.where(q == (b ^ 1), patched(b, 0), jnp.where(q == next_to(b), patched(b, 1), row))
        held.append(row)
    held = jnp.concatenate(held, axis=0)
    names = idx[q]
    small = lax.broadcasted_iota(jnp.int32, (experts, rows), 0)
    for k in range(top):
        gg_out[pl.ds(k, 1), :] = jnp.sum(
            jnp.where(small == names[k:k + 1, :], held, 0.0), axis=0, keepdims=True)
    for w in weights:
        w.wait_send()
    pl.when(end == 1)(lambda: sent_all(END))
    pl.when(end == 0)(lambda: sent_all(NEXT))
    at = part.at[pl.ds(0, 2 * dp - 1), 0]
    remote(at, at, s_p.at[0], r_p.at[0], mate).wait()
    total = part[0, c]
    for k in range(1, 2 * dp):
        total += part[k, 0]
    rg_out[...] = total


def fused(n, dp, tokens, grad_out, router_weight, expert_index, w_gate, w_up, w_down):
    rows, width = tokens.shape
    ff = w_gate.shape[2]
    top = expert_index.shape[1]
    experts = router_weight.shape[1]
    plane, cols = n // 2, width // n
    line = plane // 2
    pair = 2 * rows
    anywhere = pl.BlockSpec(memory_space=pl.ANY)
    vmem = pl.BlockSpec(memory_space=pltpu.VMEM)
    dma = pltpu.SemaphoreType.DMA
    bf, f32 = jnp.bfloat16, jnp.float32
    gg, rg = pl.pallas_call(
        functools.partial(layer_kernel, n, dp),
        out_shape=(pltpu.VMEM((top, rows), f32), pltpu.VMEM((experts, cols), f32)),
        in_specs=[anywhere] * 7,
        out_specs=(vmem, vmem),
        scratch_shapes=[
            pltpu.VMEM((line, pair, width), bf),
            pltpu.VMEM((line, pair, width), bf),
            pltpu.VMEM((experts, width), bf),
            pltpu.VMEM((plane, top, rows), jnp.int32),
            pltpu.VMEM((2, width, ff), bf),
            pltpu.VMEM((2, width, ff), bf),
            pltpu.VMEM((2, ff, width), bf),
            pltpu.VMEM((pair, ff), bf),
            pltpu.VMEM((line, 2, pair, width), bf),
            pltpu.VMEM((experts, plane * rows), f32),
            pltpu.VMEM((plane, plane + 2, 2, rows), f32),
            pltpu.VMEM((2 * dp, 2, experts, cols), f32),
            pltpu.VMEM((2, ff, width), bf),
            pltpu.VMEM((2, rows * KEPT[0] // 8, ff), bf),
            pltpu.VMEM((2, rows * KEPT[1] // 8, ff), bf),
            dma((3,)), dma((2 * plane,)), dma((2 * plane,)),
            dma((1,)), dma((1,)), dma((1,)), dma((2,)), dma((3,)), dma((3,)), dma((1,)), dma((1,)),
            dma((1,)), dma((CHUNKS,)), dma((1,)), dma((CHUNKS,)), dma((1,)), dma((1,)),
            dma((4,)), dma((4,)), dma((2,)), dma((2,)), dma((7,)),
        ],
        compiler_params=pltpu.CompilerParams(
            collective_id=0, has_side_effects=True, vmem_limit_bytes=60 * 2**20),
    )(tokens, grad_out, router_weight.T, expert_index.T, w_gate, w_up, w_down)
    def finish(a, b, x, y):
        x[...] = a[...]
        y[...] = b[...]
    gg = pltpu.with_memory_space_constraint(gg, pltpu.VMEM)
    rg = pltpu.with_memory_space_constraint(rg, pltpu.VMEM)
    gg, rg = pl.pallas_call(
        finish,
        out_shape=(jax.ShapeDtypeStruct((top, rows), f32), jax.ShapeDtypeStruct((experts, cols), f32)),
        in_specs=[vmem, vmem],
        out_specs=(vmem, vmem),
    )(gg, rg)
    return gg.T, rg.T


def solution(mesh):
    n, dp = mesh.shape["expert"], mesh.shape["dp"]

    def on_device(tokens, grad_out, router_weight, expert_index, w_gate, w_up, w_down):
        rows, width = tokens.shape
        ff = w_gate.shape[2]
        held = 2 * (2 * n // 2 * rows * width * 2 + 8 * ff * width)
        fits = n % 4 == 0 and n // 4 == 4 and dp == 2 and held < 44 * 2**20 and width % (128 * n) == 0
        fits = fits and ff % (16 * dp * CHUNKS) == 0 and ff % 128 == 0
        fits = fits and rows % 128 == 0 and router_weight.shape[1] == n
        body = functools.partial(fused, n, dp) if fits else plain
        return body(tokens, grad_out, router_weight, expert_index, w_gate, w_up, w_down)

    in_specs = (
        P(("dp", "expert"), None),
        P(("dp", "expert"), None),
        P(),
        P(("dp", "expert"), None),
        P("expert", None, None),
        P("expert", None, None),
        P("expert", None, None),
    )
    out_specs = (P(("dp", "expert"), None), P("expert", None))
    return jax.shard_map(
        on_device, mesh=mesh, in_specs=in_specs, out_specs=out_specs, check_vma=False
    )
```
